256 devices in a mesh: ta: 16 (over x, z_hi), sa: 16 (over y, z_lo, core).
Axes of the slice: x: 4, y: 4, z: 8 (z_hi: 4, z_lo: 2; z = z_hi * 2 + z_lo), core: 2. Of those that a mesh axis runs over, the one named last changes fastest.
Arguments:
- temporal_links: float32 [18, 64, 32, 384], P(None, 'ta', 'sa'), may hold values from -1 to 1, as said below
- spatial_links: float32 [3, 18, 64, 32, 384], P(None, None, 'ta', 'sa'), may hold values from -1 to 1, as said below
- rotations: float32 [3, 3, 4, 64, 32, 384], P(None, None, None, 'ta', 'sa'), may hold values from -1 to 1, as said below
Outputs:
- transfer: float32 [2, 9, 9, 16, 32, 384], P(None, None, None, 'ta', 'sa')
- log_scale: float32 [16, 32, 384], P('ta', 'sa')
The draws below stay inside these ranges and needn't reach their ends.
Inputs may be any that keep to these rules, and one draw needn't show every extreme that they name: `temporal_links`: every link's 3x3 complex matrix is special unitary. `spatial_links`: every link's 3x3 complex matrix is special unitary. `rotations`: the four entries along the third dimension form a unit quaternion.
All inputs are finite; a program needn't handle non-finite values.
Results may differ from the reference program's by a relative error of at most 0.0003.
Values sent between devices are 32-bit elements; how exact they have to be, the bound alone decides.
A program may use at most 128 MiB of HBM per device.

```python
import math
import jax
import jax.numpy as jnp
from jax import lax

SLAB = 4
SWEEPS = 3
DIST = 4
LZ = 16
NT = 64
LX = 32
LYZ = 384


def unit_quaternion(key, shape, spread):
    key_polar, key_tilt, key_turn = jax.random.split(key, 3)
    polar = jax.random.uniform(key_polar, shape, jnp.float32, 0.0, spread)
    tilt = jax.random.uniform(key_tilt, shape, jnp.float32, 0.0, math.pi)
    turn = jax.random.uniform(key_turn, shape, jnp.float32, -math.pi, math.pi)
    sine = jnp.sin(polar)
    return [jnp.cos(polar), sine * jnp.cos(tilt), sine * jnp.sin(tilt) * jnp.cos(turn), sine * jnp.sin(tilt) * jnp.sin(turn)]


def block_matrix(quaternion, upper_row, lower_row, shape):
    zeros = jnp.zeros(shape, jnp.float32)
    ones = jnp.ones(shape, jnp.float32)
    matrix = [[(ones if row_idx == col_idx else zeros, zeros) for col_idx in range(3)] for row_idx in range(3)]
    matrix[upper_row][upper_row] = (quaternion[0], quaternion[3])
    matrix[upper_row][lower_row] = (quaternion[2], quaternion[1])
    matrix[lower_row][upper_row] = (-quaternion[2], quaternion[1])
    matrix[lower_row][lower_row] = (quaternion[0], -quaternion[3])
    return matrix


def list_product(left_rows, right_rows):
    result = []
    for row_idx in range(3):
        row_list = []
        for col_idx in range(3):
            real_sum = 0.0
            imag_sum = 0.0
            for inner_idx in range(3):
                left_entry = left_rows[row_idx][inner_idx]
                right_entry = right_rows[inner_idx][col_idx]
                real_sum = real_sum + left_entry[0] * right_entry[0] - left_entry[1] * right_entry[1]
                imag_sum = imag_sum + left_entry[0] * right_entry[1] + left_entry[1] * right_entry[0]
            row_list.append((real_sum, imag_sum))
        result.append(row_list)
    return result


def special_unitary(key, shape, spread):
    keys = jax.random.split(key, 5)
    result = block_matrix(unit_quaternion(keys[0], shape, spread), 0, 1, shape)
    result = list_product(result, block_matrix(unit_quaternion(keys[1], shape, spread), 1, 2, shape))
    result = list_product(result, block_matrix(unit_quaternion(keys[2], shape, spread), 0, 1, shape))
    alpha = jax.random.uniform(keys[3], shape, jnp.float32, -spread, spread)
    beta = jax.random.uniform(keys[4], shape, jnp.float32, -spread, spread)
    zeros = jnp.zeros(shape, jnp.float32)
    phases = [[(zeros, zeros) for col_idx in range(3)] for row_idx in range(3)]
    phases[0][0] = (jnp.cos(alpha), jnp.sin(alpha))
    phases[1][1] = (jnp.cos(beta), jnp.sin(beta))
    phases[2][2] = (jnp.cos(alpha + beta), -jnp.sin(alpha + beta))
    result = list_product(result, phases)
    reals = [result[row_idx][col_idx][0] for row_idx in range(3) for col_idx in range(3)]
    imags = [result[row_idx][col_idx][1] for row_idx in range(3) for col_idx in range(3)]
    return reals + imags


def draw_temporal_links(key, part):
    spread = math.pi
    entries = special_unitary(jax.random.fold_in(key, 11), (NT, LX, LYZ), spread)
    return jnp.stack(entries, axis=0)


def draw_spatial_links(key, part):
    spread = math.pi
    entries = special_unitary(jax.random.fold_in(key, 23), (3, NT, LX, LYZ), spread)
    return jnp.stack(entries, axis=1)


def draw_rotations(key, part):
    spread = math.pi
    entries = unit_quaternion(jax.random.fold_in(key, 37), (SWEEPS, 3, NT, LX, LYZ), spread)
    return jnp.stack(entries, axis=2)


def setup_inputs(seed: int = 0) -> dict:
    key_of = jax.random.split(jax.random.key(seed), 4)
    temporal_links = draw_temporal_links(jax.random.fold_in(key_of[3], 71), 0)
    spatial_links = draw_spatial_links(jax.random.fold_in(key_of[3], 71), 0)
    rotations = draw_rotations(jax.random.fold_in(key_of[3], 71), 0)
    return {"temporal_links": temporal_links, "spatial_links": spatial_links, "rotations": rotations}


def tree_apply(function, pair):
    return (function(pair[0]), function(pair[1]))

def as_pair(links):
    shaped = links.reshape((2, 3, 3) + links.shape[1:])
    return (shaped[0], shaped[1])

def as_flat(pair):
    return jnp.stack(pair).reshape((18,) + pair[0].shape[2:])

def complex_mul(left_pair, right_pair):
    out_real = 0.0
    out_imag = 0.0
    for inner_idx in range(left_pair[0].shape[1]):
        row_real = left_pair[0][:, inner_idx:inner_idx + 1]
        row_imag = left_pair[1][:, inner_idx:inner_idx + 1]
        col_real = right_pair[0][inner_idx:inner_idx + 1]
        col_imag = right_pair[1][inner_idx:inner_idx + 1]
        out_real = out_real + row_real * col_real - row_imag * col_imag
        out_imag = out_imag + row_real * col_imag + row_imag * col_real
    return (out_real, out_imag)

def triple(first_pair, middle_pair, last_pair):
    return complex_mul(complex_mul(first_pair, middle_pair), last_pair)

def dagger(matrix):
    return (jnp.swapaxes(matrix[0], 0, 1), -jnp.swapaxes(matrix[1], 0, 1))

def add_pair(left_pair, right_pair):
    return (left_pair[0] + right_pair[0], left_pair[1] + right_pair[1])

def scalar_mul(left_pair, right_pair):
    return (left_pair[0] * right_pair[0] - left_pair[1] * right_pair[1], left_pair[0] * right_pair[1] + left_pair[1] * right_pair[0])

def shift_rows(values, offset):
    return jnp.roll(values, -offset * LZ, axis=-1)

def shift_depth(values, offset):
    position = jnp.arange(values.shape[-1]) % LZ
    if offset > 0:
        return jnp.where(position + offset >= LZ, jnp.roll(values, LZ - offset, axis=-1), jnp.roll(values, -offset, axis=-1))
    return jnp.where(position + offset < 0, jnp.roll(values, -LZ - offset, axis=-1), jnp.roll(values, -offset, axis=-1))

def later_slices(member):
    return member[:, :, 1:]

def now_slices(member):
    return member[:, :, :-1]

def rotate_rows(matrix, upper_row, lower_row, blocks):
    rows_real = [matrix[0][row_idx] for row_idx in range(3)]
    rows_imag = [matrix[1][row_idx] for row_idx in range(3)]
    upper_pair = (rows_real[upper_row], rows_imag[upper_row])
    lower_pair = (rows_real[lower_row], rows_imag[lower_row])
    new_upper = add_pair(scalar_mul(blocks[0], upper_pair), scalar_mul(blocks[1], lower_pair))
    new_lower = add_pair(scalar_mul(blocks[2], upper_pair), scalar_mul(blocks[3], lower_pair))
    rows_real[upper_row] = new_upper[0]
    rows_imag[upper_row] = new_upper[1]
    rows_real[lower_row] = new_lower[0]
    rows_imag[lower_row] = new_lower[1]
    return (jnp.stack(rows_real), jnp.stack(rows_imag))

def relax(temporal, center, left_x, rotation, parity, first_col):
    col_count = rotation.shape[3]
    own_links = tree_apply(lambda member: member[..., 1:col_count + 1, :], temporal)
    ahead_links = tree_apply(lambda member: member[..., 2:col_count + 2, :], temporal)
    behind = tree_apply(lambda member: member[..., 0:col_count, :], temporal)
    staple = add_pair(triple(tree_apply(later_slices, center[0]), dagger(ahead_links), dagger(tree_apply(now_slices, center[0]))), triple(dagger(tree_apply(later_slices, left_x)), dagger(behind), tree_apply(now_slices, left_x)))
    for direction, shifter in ((1, shift_rows), (2, shift_depth)):
        side_link = center[direction]
        back_link = tree_apply(lambda member: shifter(member, -1), side_link)
        forward_time = tree_apply(lambda member: shifter(member, 1), own_links)
        backward_time = tree_apply(lambda member: shifter(member, -1), own_links)
        staple = add_pair(staple, add_pair(triple(tree_apply(later_slices, side_link), dagger(forward_time), dagger(tree_apply(now_slices, side_link))), triple(dagger(tree_apply(later_slices, back_link)), dagger(backward_time), tree_apply(now_slices, back_link))))
    product = complex_mul(own_links, staple)
    updated = own_links
    for subgroup, (upper_row, lower_row) in enumerate(((0, 1), (1, 2), (0, 2))):
        prod_real, prod_imag = product
        stat_zero = 0.5 * (prod_real[upper_row, upper_row] + prod_real[lower_row, lower_row])
        stat_one = 0.5 * (prod_imag[upper_row, lower_row] + prod_imag[lower_row, upper_row])
        stat_two = 0.5 * (prod_real[upper_row, lower_row] - prod_real[lower_row, upper_row])
        stat_three = 0.5 * (prod_imag[upper_row, upper_row] - prod_imag[lower_row, lower_row])
        vec_sq = stat_one * stat_one + stat_two * stat_two + stat_three * stat_three
        norm_sq = jnp.maximum(stat_zero * stat_zero + vec_sq, 0.5)
        refl_zero = (stat_zero * stat_zero - vec_sq) / norm_sq
        refl_one = -2.0 * stat_zero * stat_one / norm_sq
        refl_two = -2.0 * stat_zero * stat_two / norm_sq
        refl_three = -2.0 * stat_zero * stat_three / norm_sq
        turn_zero = rotation[subgroup, 0]
        turn_one = rotation[subgroup, 1]
        turn_two = rotation[subgroup, 2]
        turn_three = rotation[subgroup, 3]
        new_zero = turn_zero * refl_zero - (turn_one * refl_one + turn_two * refl_two + turn_three * refl_three)
        new_one = turn_zero * refl_one + refl_zero * turn_one - (turn_two * refl_three - turn_three * refl_two)
        new_two = turn_zero * refl_two + refl_zero * turn_two - (turn_three * refl_one - turn_one * refl_three)
        new_three = turn_zero * refl_three + refl_zero * turn_three - (turn_one * refl_two - turn_two * refl_one)
        blocks = ((new_zero, new_three), (new_two, new_one), (-new_two, new_one), (new_zero, -new_three))
        updated = rotate_rows(updated, upper_row, lower_row, blocks)
        product = rotate_rows(product, upper_row, lower_row, blocks)
    col_pos = first_col + jnp.arange(col_count)
    flat_pos = jnp.arange(own_links[0].shape[-1])
    parity_mask = (col_pos[:, None] + flat_pos[None, :] // LZ + flat_pos[None, :] % LZ) % 2 == parity
    return (jnp.where(parity_mask, updated[0], own_links[0]), jnp.where(parity_mask, updated[1], own_links[1]))

def slab_operator(links):
    product = tree_apply(lambda member: member[:, :, 0], links)
    for time_idx in range(1, links[0].shape[2]):
        product = complex_mul(product, tree_apply(lambda member: member[:, :, time_idx], links))
    partner = tree_apply(lambda member: shift_depth(member, DIST), product)
    col_count = product[0].shape[2]
    site_count = product[0].shape[3]
    left_real = product[0][:, None, :, None]
    left_imag = product[1][:, None, :, None]
    right_real = partner[0][None, :, None, :]
    right_imag = partner[1][None, :, None, :]
    real_part = (left_real * right_real + left_imag * right_imag).reshape(9, 9, col_count, site_count)
    imag_part = (left_imag * right_real - left_real * right_imag).reshape(9, 9, col_count, site_count)
    return (real_part, imag_part)

def normalize(real_part, imag_part):
    mean_sq = (lax.optimization_barrier(jnp.sum(real_part * real_part, axis=(0, 1))) + lax.optimization_barrier(jnp.sum(imag_part * imag_part, axis=(0, 1)))) / 162.0
    rms_scale = jnp.sqrt(mean_sq + 1e-06)
    return (real_part / rms_scale, imag_part / rms_scale, jnp.log(rms_scale))

def chain_combine(earlier, later):
    prod_real, prod_imag = complex_mul((earlier[0], earlier[1]), (later[0], later[1]))
    real_part, imag_part, extra_log = normalize(prod_real, prod_imag)
    return (real_part, imag_part, earlier[2] + later[2] + extra_log)

def slab_pass(inputs):
    temporal, spatial_ext, rotation = inputs
    center = [as_pair(spatial_ext[dir_idx]) for dir_idx in range(3)]
    left_x = as_pair(jnp.roll(spatial_ext[0], 1, axis=2))
    current = temporal
    for sweep_idx in range(SWEEPS):
        for parity in (0, 1):
            padded = jnp.concatenate([current[:, :, -1:], current, current[:, :, :1]], axis=2)
            current = as_flat(relax(as_pair(padded), center, left_x, rotation[sweep_idx], parity, 0))
        real_part, imag_part = slab_operator(as_pair(current))
        if sweep_idx == 0:
            total_real, total_imag = (real_part, imag_part)
        else:
            total_real = total_real + real_part
            total_imag = total_imag + imag_part
    return normalize(total_real * (1.0 / SWEEPS), total_imag * (1.0 / SWEEPS))

def reference(temporal_links, spatial_links, rotations):
    slab_count = NT // SLAB
    temporal_slabs = jnp.moveaxis(temporal_links.reshape(18, slab_count, SLAB, LX, LYZ), 1, 0)
    spatial_slabs = spatial_links.reshape(3, 18, slab_count, SLAB, LX, LYZ)
    next_first = jnp.roll(spatial_slabs[:, :, :, 0:1], -1, axis=2)
    spatial_ext = jnp.moveaxis(jnp.concatenate([spatial_slabs, next_first], axis=3), 2, 0)
    rotation_slabs = jnp.moveaxis(rotations.reshape(SWEEPS, 3, 4, slab_count, SLAB, LX, LYZ), 3, 0)
    averaged = lax.map(slab_pass, (temporal_slabs, spatial_ext, rotation_slabs))
    eye_real = jnp.broadcast_to(jnp.eye(9, dtype=temporal_links.dtype)[:, :, None, None], (9, 9, LX, LYZ))
    initial = (eye_real, jnp.zeros_like(eye_real), jnp.zeros((LX, LYZ), temporal_links.dtype))

    def advance(carry, piece):
        combined = chain_combine(carry, piece)
        return (combined, combined)
    final_state, chain_all = lax.scan(advance, initial, averaged)
    transfer = jnp.stack([jnp.moveaxis(chain_all[0], 0, 2), jnp.moveaxis(chain_all[1], 0, 2)])
    return (transfer, chain_all[2])
```

```python
import jax
import jax.numpy as jnp
from jax import lax
from jax.experimental import pallas as pl
from jax.experimental.pallas import tpu as pltpu
from jax.sharding import Mesh
from jax.sharding import PartitionSpec as P

SWEEPS = 3
LZ = 16
LANES = 128
MESH = pl.DeviceIdType.MESH
AXES = ("ta_0", "ta_1", "sa")
PLANES = ((0, 1), (1, 2), (0, 2))


def times(left, right):
    out_re, out_im = [], []
    for row in range(3):
        for col in range(3):
            re = im = None
            for mid in range(3):
                a_re, a_im = left[0][3 * row + mid], left[1][3 * row + mid]
                b_re, b_im = right[0][3 * mid + col], right[1][3 * mid + col]
                p_re = a_re * b_re - a_im * b_im
                p_im = a_re * b_im + a_im * b_re
                re = p_re if re is None else re + p_re
                im = p_im if im is None else im + p_im
            out_re.append(re)
            out_im.append(im)
    return out_re, out_im


def staple_term(total, later, now, link):
    total_re, total_im = list(total[0]), list(total[1])
    for col in range(3):
        mid_re, mid_im = [], []
        for k in range(3):
            re = im = None
            for m in range(3):
                a_re, a_im = now[0][3 * col + m], now[1][3 * col + m]
                b_re, b_im = link[0][3 * m + k], link[1][3 * m + k]
                p_re = a_re * b_re - a_im * b_im
                p_im = a_re * b_im + a_im * b_re
                re = p_re if re is None else re + p_re
                im = p_im if im is None else im + p_im
            mid_re.append(re)
            mid_im.append(im)
        for row in range(3):
            re, im = total_re[3 * row + col], total_im[3 * row + col]
            for k in range(3):
                a_re, a_im = later[0][3 * row + k], later[1][3 * row + k]
                p_re = a_re * mid_re[k] + a_im * mid_im[k]
                p_im = a_im * mid_re[k] - a_re * mid_im[k]
                re = p_re if re is None else re + p_re
                im = p_im if im is None else im + p_im
            total_re[3 * row + col], total_im[3 * row + col] = re, im
    return total_re, total_im


def dagger(matrix):
    order = (0, 3, 6, 1, 4, 7, 2, 5, 8)
    return [matrix[0][k] for k in order], [-matrix[1][k] for k in order]


def rotate_rows(matrix, upper, lower, quat):
    q0, q1, q2, q3 = quat
    re, im = list(matrix[0]), list(matrix[1])
    for col in range(3):
        u_re, u_im = matrix[0][3 * upper + col], matrix[1][3 * upper + col]
        l_re, l_im = matrix[0][3 * lower + col], matrix[1][3 * lower + col]
        re[3 * upper + col] = q0 * u_re - q3 * u_im + q2 * l_re - q1 * l_im
        im[3 * upper + col] = q0 * u_im + q3 * u_re + q2 * l_im + q1 * l_re
        re[3 * lower + col] = q0 * l_re + q3 * l_im - q2 * u_re - q1 * u_im
        im[3 * lower + col] = q0 * l_im - q3 * l_re - q2 * u_im + q1 * u_re
    return re, im


def reflected(product, upper, lower, turn):
    re, im = product
    uu, ul, lu, ll = 4 * upper, 3 * upper + lower, 3 * lower + upper, 4 * lower
    w0 = 0.5 * (re[uu] + re[ll])
    w1 = 0.5 * (im[ul] + im[lu])
    w2 = 0.5 * (re[ul] - re[lu])
    w3 = 0.5 * (im[uu] - im[ll])
    vec_sq = w1 * w1 + w2 * w2 + w3 * w3
    w0_sq = w0 * w0
    inv = 1.0 / jnp.maximum(w0_sq + vec_sq, 0.5)
    scale = -2.0 * w0 * inv
    r0, r1, r2, r3 = (w0_sq - vec_sq) * inv, scale * w1, scale * w2, scale * w3
    x0, x1, x2, x3 = turn
    return (
        x0 * r0 - (x1 * r1 + x2 * r2 + x3 * r3),
        x0 * r1 + r0 * x1 - (x2 * r3 - x3 * r2),
        x0 * r2 + r0 * x2 - (x3 * r1 - x1 * r3),
        x0 * r3 + r0 * x3 - (x1 * r2 - x2 * r1),
    )


def turn_lanes(value, steps):
    return pltpu.roll(value, (-steps) % LANES, 1)


def turn_rows(value, steps):
    return pltpu.roll(value, (-steps) % 8, 0)


class Shifts:
    def __init__(self):
        lane = lax.broadcasted_iota(jnp.int32, (8, LANES), 1)
        row = lax.broadcasted_iota(jnp.int32, (8, LANES), 0)
        self.depth = lane % LZ
        self.lane = lane
        self.slot = row % 4
        self.odd = ((lane // LZ + lane) % 2) == 1
        self.low_rows = row < 4
        self.even_lane = lane % 2 == 0

    def rows(self, value, offset):
        if offset > 0:
            turned = turn_lanes(value, LZ)
            after = jnp.where(self.slot == 2, turn_rows(turned, -2), turn_rows(turned, 1))
            return jnp.where(self.lane < LANES - LZ, turned, after)
        turned = turn_lanes(value, -LZ)
        before = jnp.where(self.slot == 0, turn_rows(turned, 2), turn_rows(turned, -1))
        return jnp.where(self.lane >= LZ, turned, before)

    def deep(self, value, offset):
        if offset > 0:
            return jnp.where(
                self.depth < LZ - offset, turn_lanes(value, offset), turn_lanes(value, offset - LZ)
            )
        return jnp.where(
            self.depth >= -offset, turn_lanes(value, offset), turn_lanes(value, LZ + offset)
        )

    def pair_swap(self, value):
        return jnp.where(self.even_lane, turn_lanes(value, 1), turn_lanes(value, -1))


def kernel(
    time_hbm, space_hbm, turn_hbm, out_ref,
    time_raw, space_raw, left_raw, halo_raw, turn_raw,
    field, bonds, shifted, pack_out, pack_in, loop_rows, loop_out, loop_in,
    oper, chain_a, chain_b, group, part, final,
    in_sem, edge_out, edge_in, halo_out, halo_in, loop_sent, loop_got, local_sem, back_sem, done_sem,
):
    ix, iz, ia = lax.axis_index("ta_0"), lax.axis_index("ta_1"), lax.axis_index("sa")
    nx, nz, na = 4, 4, lax.axis_size("sa")
    left, right = lax.rem(ia + na - 1, na), lax.rem(ia + 1, na)
    slab = ix * nz + iz
    earlier = lax.rem(slab + nx * nz - 1, nx * nz)
    later = lax.rem(slab + 1, nx * nz)
    earlier_x, earlier_z = earlier // nz, lax.rem(earlier, nz)
    later_x, later_z = later // nz, lax.rem(later, nz)

    local = []
    for t in range(4):
        for j in range(3):
            lanes, rows = pl.ds(LANES * j, LANES), pl.ds(8 * t + 2 * j, 2)
            local.append(pltpu.make_async_copy(
                time_hbm.at[:, t, :, lanes], time_raw.at[:, rows, :], in_sem.at[0]))
            local.append(pltpu.make_async_copy(
                space_hbm.at[:, :, t, :, lanes], space_raw.at[:, :, rows, :], in_sem.at[1]))
            local.append(pltpu.make_async_copy(
                turn_hbm.at[:, :, :, t, :, lanes], turn_raw.at[:, :, :, rows, :], in_sem.at[2]))
    for copy in local:
        copy.start()

    barrier = pltpu.get_barrier_semaphore()
    peers = []
    for step in range(1, nx * nz):
        peer = lax.rem(slab + step, nx * nz)
        peers.append((peer // nz, lax.rem(peer, nz), ia))
    peers += [(ix, iz, left), (ix, iz, right)]
    peers += [(earlier_x, earlier_z, right), (later_x, later_z, left)]
    for peer in peers:
        pl.semaphore_signal(barrier, inc=1, device_id=peer, device_id_type=MESH)
    pl.semaphore_wait(barrier, len(peers))

    def remote(src, dst, out_sem, got_sem, target):
        return pltpu.make_async_remote_copy(
            src_ref=src, dst_ref=dst, send_sem=out_sem, recv_sem=got_sem,
            device_id=target, device_id_type=MESH)

    def edge(group, src, dst, target):
        return remote(src, dst, edge_out.at[group], edge_in.at[group], target)

    def landed(ref, sem):
        pltpu.make_async_copy(ref, ref, sem).wait()

    edges = []
    for t in range(4):
        for j in range(3):
            lanes = pl.ds(LANES * j, LANES)
            low, high = pl.ds(8 * t + 2 * j, 1), pl.ds(8 * t + 2 * j + 1, 1)
            edges.append(edge(
                0, time_hbm.at[:, t, pl.ds(0, 1), lanes], halo_raw.at[:, low, :], (ix, iz, left)))
            edges.append(edge(
                1, time_hbm.at[:, t, pl.ds(1, 1), lanes], halo_raw.at[:, high, :], (ix, iz, right)))
            edges.append(edge(
                2, space_hbm.at[0, :, t, pl.ds(1, 1), lanes], left_raw.at[:, high, :],
                (ix, iz, right)))
    for j in range(3):
        lanes = pl.ds(LANES * j, LANES)
        edges.append(edge(
            3, space_hbm.at[:, :, 0, :, lanes], space_raw.at[:, :, pl.ds(32 + 2 * j, 2), :],
            (earlier_x, earlier_z, ia)))
        edges.append(edge(
            4, space_hbm.at[0, :, 0, pl.ds(1, 1), lanes],
            left_raw.at[:, pl.ds(32 + 2 * j + 1, 1), :], (earlier_x, earlier_z, right)))
    covers = (
        halo_raw.at[:, pl.ds(0, 12), :], halo_raw.at[:, pl.ds(0, 12), :],
        halo_raw.at[:, pl.ds(0, 12), :], space_raw.at[:, :, pl.ds(0, 6), :],
        halo_raw.at[:, pl.ds(0, 3), :])
    for copy in edges:
        copy.start()

    shifts = Shifts()
    odd = shifts.odd

    def own(parity, first, second):
        return jnp.where(odd, first, second) if parity else jnp.where(odd, second, first)

    landed(time_raw.at[:, pl.ds(0, 24), :], in_sem.at[0])
    landed(space_raw.at[:, :, pl.ds(0, 24), :], in_sem.at[1])
    landed(turn_raw.at[:, :, :, pl.ds(0, 24), :], in_sem.at[2])
    for block in range(2):
        for entry in range(18):
            first = time_raw[entry, pl.ds(16 * block, 8, stride=2), :]
            second = time_raw[entry, pl.ds(16 * block + 1, 8, stride=2), :]
            field[0, entry, pl.ds(8 * block, 8), :] = own(0, first, second)
            field[1, entry, pl.ds(8 * block, 8), :] = own(1, first, second)
    for group_idx, cover in enumerate(covers):
        landed(cover, edge_in.at[group_idx])

    @pl.loop(0, 3)
    def _(block):
        at = pl.multiple_of(16 * block, 16)
        to = pl.ds(pl.multiple_of(8 * block, 8), 8)

        def raw(ref, lead, column):
            return [ref[(*lead, k, pl.ds(at + column, 8, stride=2), slice(None))] for k in range(18)]

        def put(parity, place, matrix):
            for k in range(9):
                bonds[parity, place, k, to, :] = matrix[0][k]
                bonds[parity, place, 9 + k, to, :] = matrix[1][k]

        def split(values):
            return values[:9], values[9:]

        inner, outer, beyond = (
            raw(space_raw, (0,), 0), raw(space_raw, (0,), 1), raw(left_raw, (), 1))
        inner_dag, beyond_dag = dagger(split(inner)), dagger(split(beyond))
        inner_dag, beyond_dag = inner_dag[0] + inner_dag[1], beyond_dag[0] + beyond_dag[1]
        for parity in (0, 1):
            put(parity, 0, split([own(parity, a, b) for a, b in zip(inner, inner_dag)]))
            put(parity, 5, split([own(parity, a, b) for a, b in zip(beyond_dag, outer)]))
        for direction, shift in ((1, shifts.rows), (2, shifts.deep)):
            first, second = raw(space_raw, (direction,), 0), raw(space_raw, (direction,), 1)
            for parity in (0, 1):
                here = [own(parity, a, b) for a, b in zip(first, second)]
                put(parity, 2 * direction - 1, split(here))
                back = [shift(value, -1) for value in here]
                put(1 - parity, 2 * direction, dagger(split(back)))

    def half_sweep(sweep, parity):
        number = 2 * sweep + parity

        @pl.loop(0, 2)
        def _(block):
            rows = pl.ds(pl.multiple_of(8 * block, 8), 8)
            rows_later = pl.ds(8 * block + 4, 8)

            def load(ref, lead, where):
                values = [ref[(*lead, k, where, slice(None))] for k in range(18)]
                return values[:9], values[9:]

            for entry in range(18):
                value = field[1 - parity, entry, rows, :]
                shifted[0, entry] = shifts.rows(value, 1)
                shifted[1, entry] = shifts.rows(value, -1)
                shifted[2, entry] = shifts.deep(value, 1)
                shifted[3, entry] = shifts.deep(value, -1)
            total = ([None] * 9, [None] * 9)
            total = staple_term(
                total, load(bonds, (parity, 0), rows_later), load(bonds, (parity, 0), rows),
                load(field, (1 - parity,), rows))
            for place in range(1, 5):
                total = staple_term(
                    total, load(bonds, (parity, place), rows_later),
                    load(bonds, (parity, place), rows),
                    load(shifted, (place - 1,), slice(None)))
            for k in range(9):
                shifted[4, k] = total[0][k]
                shifted[4, 9 + k] = total[1][k]

            @pl.when(number == 0)
            def _():
                base = pl.multiple_of(16 * block, 16)
                for entry in range(18):
                    from_right = halo_raw[entry, pl.ds(base, 8, stride=2), :]
                    from_left = halo_raw[entry, pl.ds(base + 1, 8, stride=2), :]
                    shifted[5, entry] = own(parity, from_left, from_right)

            @pl.when(number > 0)
            def _():
                for side in range(2):
                    remote(
                        pack_out.at[number - 1, block, side], pack_in.at[number - 1, block, side],
                        halo_out.at[number - 1, block, side], halo_in.at[number - 1, block, side],
                        (ix, iz, left)).wait_recv()
                for k in range(9):
                    from_left = pack_in[number - 1, block, 1, k]
                    from_right = pack_in[number - 1, block, 0, k]
                    shifted[5, k] = own(parity, from_left, from_right)
                    shifted[5, 9 + k] = shifts.pair_swap(own(parity, from_right, from_left))

            total = load(shifted, (4,), slice(None))
            total = staple_term(
                total, load(bonds, (parity, 5), rows_later), load(bonds, (parity, 5), rows),
                load(shifted, (5,), slice(None)))
            links = load(field, (parity,), rows)
            product = times(links, total)
            for plane, (upper, lower) in enumerate(PLANES):
                base = pl.multiple_of(16 * block, 16)
                turn = [
                    own(parity, turn_raw[sweep, plane, k, pl.ds(base, 8, stride=2), :],
                        turn_raw[sweep, plane, k, pl.ds(base + 1, 8, stride=2), :])
                    for k in range(4)]
                quat = reflected(product, upper, lower, turn)
                links = rotate_rows(links, upper, lower, quat)
                if plane < 2:
                    product = rotate_rows(product, upper, lower, quat)
            for k in range(9):
                field[parity, k, rows, :] = links[0][k]
                field[parity, 9 + k, rows, :] = links[1][k]

            @pl.when(number < 2 * SWEEPS - 1)
            def _():
                for k in range(9):
                    real, partner = links[0][k], shifts.pair_swap(links[1][k])
                    pack_out[number, block, 0, k] = own(parity, real, partner)
                    pack_out[number, block, 1, k] = own(parity, partner, real)
                for side, target in ((0, left), (1, right)):
                    remote(
                        pack_out.at[number, block, side], pack_in.at[number, block, side],
                        halo_out.at[number, block, side], halo_in.at[number, block, side],
                        (ix, iz, target)).start()

    def send_loops(sweep):
        low = shifts.low_rows
        stage = []
        for parity in (0, 1):
            even, odd_t = [], []
            for entry in range(18):
                a = field[parity, entry, pl.ds(0, 8), :]
                b = field[parity, entry, pl.ds(4, 8), :]
                c = field[parity, entry, pl.ds(8, 8), :]
                even.append(jnp.where(low, a, b))
                odd_t.append(jnp.where(low, b, c))
            stage.append(times((even[:9], even[9:]), (odd_t[:9], odd_t[9:])))
        head, tail = [], []
        for part_idx in (0, 1):
            for k in range(9):
                a, b = stage[0][part_idx][k], stage[1][part_idx][k]
                head.append(jnp.where(low, a, turn_rows(b, 4)))
                tail.append(jnp.where(low, turn_rows(a, 4), b))
        loops = times((head[:9], head[9:]), (tail[:9], tail[9:]))
        for entry, value in enumerate(loops[0] + loops[1]):
            loop_rows[entry] = own(0, value, turn_rows(value, 4))
            for j in range(4):
                loop_out[sweep, entry, pl.ds(2 * j, 2), :] = (
                    loop_rows[entry, pl.ds(j, 2, stride=4), :])
        for step in range(nx * nz):
            if step == 0:
                @pl.when(ix > 0)
                def _():
                    pltpu.make_async_copy(
                        loop_out.at[sweep, :, pl.ds(2 * (ix - 1), 2), :],
                        loop_in.at[sweep, iz, :, pl.ds(2 * ix, 2), :], local_sem.at[sweep]).start()
            else:
                peer = lax.rem(slab + step, nx * nz)
                peer_x, peer_z = peer // nz, lax.rem(peer, nz)

                @pl.when(peer_x > 0)
                def _():
                    remote(
                        loop_out.at[sweep, :, pl.ds(2 * (peer_x - 1), 2), :],
                        loop_in.at[sweep, iz, :, pl.ds(2 * ix, 2), :],
                        loop_sent.at[sweep], loop_got.at[sweep], (peer_x, peer_z, ia)).start()

    @pl.loop(0, SWEEPS)
    def _(sweep):
        half_sweep(sweep, 0)
        half_sweep(sweep, 1)
        send_loops(sweep)

    def normalized(load, store, log):
        square = None
        for k in range(162):
            value = load(k)
            square = value * value if square is None else square + value * value
        rms = jnp.sqrt(square / 162.0 + 1e-06)
        inv = 1.0 / rms
        for k in range(162):
            store(k, load(k) * inv)
        return log + jnp.log(rms)

    def combine(left_ref, right_ref, dst_ref, keep):
        @pl.loop(0, 9)
        def _(row):
            for half in range(3):
                columns = range(3 * half, 3 * half + 3)
                re, im = [None] * 3, [None] * 3
                for mid in range(9):
                    a_re, a_im = left_ref[9 * row + mid], left_ref[81 + 9 * row + mid]
                    for place, col in enumerate(columns):
                        b_re, b_im = right_ref[9 * mid + col], right_ref[81 + 9 * mid + col]
                        p_re = a_re * b_re - a_im * b_im
                        p_im = a_re * b_im + a_im * b_re
                        re[place] = p_re if re[place] is None else re[place] + p_re
                        im[place] = p_im if im[place] is None else im[place] + p_im
                for place, col in enumerate(columns):
                    dst_ref[9 * row + col] = re[place]
                    dst_ref[81 + 9 * row + col] = im[place]
        log = normalized(
            lambda k: dst_ref[k], lambda k, value: dst_ref.__setitem__(k, keep(k, value)),
            left_ref[162] + right_ref[162])
        dst_ref[162] = keep(162, log)

    @pl.when(ix > 0)
    def _():
        for sweep in range(SWEEPS):
            pltpu.make_async_copy(
                loop_out.at[sweep, :, pl.ds(2 * (ix - 1), 2), :],
                loop_in.at[sweep, iz, :, pl.ds(2 * ix, 2), :], local_sem.at[sweep]).wait()
            landed(space_raw.at[0, :, pl.ds(0, 30), :], loop_got.at[sweep])

        @pl.loop(0, nz)
        def _(slot):
            for sweep in range(SWEEPS):
                loops = [loop_in[sweep, slot, k] for k in range(18)]
                partner = [shifts.deep(value, 4) for value in loops]
                for a in range(3):
                    for c in range(3):
                        for e in range(3):
                            for d in range(3):
                                l_re, l_im = loops[3 * a + e], loops[9 + 3 * a + e]
                                r_re, r_im = partner[3 * c + d], partner[9 + 3 * c + d]
                                re = l_re * r_re + l_im * r_im
                                im = l_im * r_re - l_re * r_im
                                at = 9 * (3 * a + c) + 3 * e + d
                                if sweep:
                                    re = oper[slot, at] + re
                                    im = oper[slot, 81 + at] + im
                                oper[slot, at] = re
                                oper[slot, 81 + at] = im
            third = 1.0 / SWEEPS
            log = normalized(
                lambda k: oper[slot, k] * third,
                lambda k, value: oper.at[slot].__setitem__(k, value), jnp.zeros((8, LANES)))
            oper[slot, 162] = log

        @pl.loop(0, 163)
        def _(k):
            part[0, k] = oper[0, k]

        @pl.loop(1, nz)
        def _(slot):
            combine(part.at[slot - 1], oper.at[slot], part.at[slot], lambda k, value: value)

        row = lax.broadcasted_iota(jnp.int32, (8, LANES), 0)

        def moved(value, k, rows):
            unit = 1.0 if k < 81 and k % 10 == 0 else 0.0
            return jnp.where(row < rows, unit, turn_rows(value, -rows))

        for k in range(163):
            chain_a[k] = moved(part[nz - 1, k], k, 2)
            chain_b[k] = moved(chain_a[k], k, 2)
        combine(chain_b, chain_a, group, lambda k, value: jnp.where(row < 2, chain_a[k], value))
        for k in range(163):
            chain_b[k] = moved(group[k], k, 4)
        combine(chain_b, group, chain_a, lambda k, value: jnp.where(row < 4, group[k], value))
        combine(chain_a, part.at[iz], final, lambda k, value: value)

        for target in range(nx):
            src = final.at[:, pl.ds(2 * target, 2), :]
            dst = out_ref.at[:, ix - 1]

            @pl.when(ix == target)
            def _():
                pltpu.make_async_copy(src, dst, done_sem.at[0]).start()

            @pl.when(ix != target)
            def _():
                pltpu.make_async_remote_copy(
                    src_ref=src, dst_ref=dst, send_sem=done_sem.at[1], recv_sem=back_sem.at[ix],
                    device_id=(target, iz, ia), device_id_type=MESH).start()
        pltpu.make_async_copy(
            final.at[:, pl.ds(0, 2), :], out_ref.at[:, 0], done_sem.at[0]).wait()

    for source in range(1, nx):
        @pl.when(ix != source)
        def _():
            remote(
                final.at[:, pl.ds(0, 2), :], out_ref.at[:, 0], done_sem.at[1], back_sem.at[source],
                (ix, iz, left)).wait_recv()

    for group_idx, cover in enumerate(covers):
        landed(cover, edge_out.at[group_idx])
    for number in range(2 * SWEEPS - 1):
        for block in range(2):
            for side in range(2):
                landed(pack_out.at[number, block, side], halo_out.at[number, block, side])

    @pl.when(ix == 0)
    def _():
        for sweep in range(SWEEPS):
            landed(space_raw.at[0, :, pl.ds(0, 24), :], loop_sent.at[sweep])

    @pl.when(ix > 0)
    def _():
        for sweep in range(SWEEPS):
            landed(space_raw.at[0, :, pl.ds(0, 22), :], loop_sent.at[sweep])
        landed(final.at[:, pl.ds(0, 6), :], done_sem.at[1])


def per_device(temporal_links, spatial_links, rotations):
    f32, dma = jnp.float32, pltpu.SemaphoreType.DMA
    halves = 2 * SWEEPS - 1
    out = pl.pallas_call(
        kernel,
        name="slab_chain",
        out_shape=jax.ShapeDtypeStruct((163, 3, 2, LANES), f32),
        in_specs=[pl.BlockSpec(memory_space=pl.ANY)] * 3,
        out_specs=pl.BlockSpec(memory_space=pltpu.VMEM),
        scratch_shapes=[
            pltpu.VMEM((18, 32, LANES), f32),
            pltpu.VMEM((3, 18, 48, LANES), f32),
            pltpu.VMEM((18, 48, LANES), f32),
            pltpu.VMEM((18, 32, LANES), f32),
            pltpu.VMEM((3, 3, 4, 32, LANES), f32),
            pltpu.VMEM((2, 18, 16, LANES), f32),
            pltpu.VMEM((2, 6, 18, 24, LANES), f32),
            pltpu.VMEM((6, 18, 8, LANES), f32),
            pltpu.VMEM((halves, 2, 2, 9, 8, LANES), f32),
            pltpu.VMEM((halves, 2, 2, 9, 8, LANES), f32),
            pltpu.VMEM((18, 8, LANES), f32),
            pltpu.VMEM((SWEEPS, 18, 8, LANES), f32),
            pltpu.VMEM((SWEEPS, 4, 18, 8, LANES), f32),
            pltpu.VMEM((4, 163, 8, LANES), f32),
            pltpu.VMEM((163, 8, LANES), f32),
            pltpu.VMEM((163, 8, LANES), f32),
            pltpu.VMEM((163, 8, LANES), f32),
            pltpu.VMEM((4, 163, 8, LANES), f32),
            pltpu.VMEM((163, 8, LANES), f32),
            dma((3,)), dma((5,)), dma((5,)), dma((halves, 2, 2)), dma((halves, 2, 2)),
            dma((SWEEPS,)), dma((SWEEPS,)), dma((SWEEPS,)), dma((4,)), dma((2,)),
        ],
        compiler_params=pltpu.CompilerParams(collective_id=0, has_side_effects=True),
    )(temporal_links, spatial_links, rotations)
    transfer = out[:162].reshape(2, 9, 9, 3, 2, LANES).transpose(0, 1, 2, 4, 3, 5)
    log_scale = out[162].transpose(1, 0, 2).reshape(1, 2, 3 * LANES)
    return transfer.reshape(2, 9, 9, 1, 2, 3 * LANES), log_scale


def solution(mesh):
    split = Mesh(mesh.devices.reshape(4, 4, mesh.shape["sa"]), AXES)
    slabs = ("ta_0", "ta_1")
    return jax.shard_map(
        per_device,
        mesh=split,
        in_specs=(
            P(None, slabs, "sa", None),
            P(None, None, slabs, "sa", None),
            P(None, None, None, slabs, "sa", None),
        ),
        out_specs=(P(None, None, None, slabs, "sa", None), P(slabs, "sa", None)),
        check_vma=False,
    )
```

```python
import jax
import jax.numpy as jnp
from jax import lax
from jax.experimental import pallas as pl
from jax.experimental.pallas import tpu as pltpu
from jax.sharding import Mesh
from jax.sharding import PartitionSpec as P

SWEEPS = 3
LZ = 16
LANES = 128
MESH = pl.DeviceIdType.MESH
AXES = ("ta_0", "ta_1", "sa")
PLANES = ((0, 1), (1, 2), (0, 2))


def times(left, right):
    out_re, out_im = [], []
    for row in range(3):
        for col in range(3):
            re = im = None
            for mid in range(3):
                a_re, a_im = left[0][3 * row + mid], left[1][3 * row + mid]
                b_re, b_im = right[0][3 * mid + col], right[1][3 * mid + col]
                p_re = a_re * b_re - a_im * b_im
                p_im = a_re * b_im + a_im * b_re
                re = p_re if re is None else re + p_re
                im = p_im if im is None else im + p_im
            out_re.append(re)
            out_im.append(im)
    return out_re, out_im


def staple_term(total, later, now, link):
    total_re, total_im = list(total[0]), list(total[1])
    for col in range(3):
        mid_re, mid_im = [], []
        for k in range(3):
            re = im = None
            for m in range(3):
                a_re, a_im = now[0][3 * col + m], now[1][3 * col + m]
                b_re, b_im = link[0][3 * m + k], link[1][3 * m + k]
                p_re = a_re * b_re - a_im * b_im
                p_im = a_re * b_im + a_im * b_re
                re = p_re if re is None else re + p_re
                im = p_im if im is None else im + p_im
            mid_re.append(re)
            mid_im.append(im)
        for row in range(3):
            re, im = total_re[3 * row + col], total_im[3 * row + col]
            for k in range(3):
                a_re, a_im = later[0][3 * row + k], later[1][3 * row + k]
                p_re = a_re * mid_re[k] + a_im * mid_im[k]
                p_im = a_im * mid_re[k] - a_re * mid_im[k]
                re = p_re if re is None else re + p_re
                im = p_im if im is None else im + p_im
            total_re[3 * row + col], total_im[3 * row + col] = re, im
    return total_re, total_im


def dagger(matrix):
    order = (0, 3, 6, 1, 4, 7, 2, 5, 8)
    return [matrix[0][k] for k in order], [-matrix[1][k] for k in order]


def rotate_rows(matrix, upper, lower, quat):
    q0, q1, q2, q3 = quat
    re, im = list(matrix[0]), list(matrix[1])
    for col in range(3):
        u_re, u_im = matrix[0][3 * upper + col], matrix[1][3 * upper + col]
        l_re, l_im = matrix[0][3 * lower + col], matrix[1][3 * lower + col]
        re[3 * upper + col] = q0 * u_re - q3 * u_im + q2 * l_re - q1 * l_im
        im[3 * upper + col] = q0 * u_im + q3 * u_re + q2 * l_im + q1 * l_re
        re[3 * lower + col] = q0 * l_re + q3 * l_im - q2 * u_re - q1 * u_im
        im[3 * lower + col] = q0 * l_im - q3 * l_re - q2 * u_im + q1 * u_re
    return re, im


def reflected(product, upper, lower, turn):
    re, im = product
    uu, ul, lu, ll = 4 * upper, 3 * upper + lower, 3 * lower + upper, 4 * lower
    w0 = 0.5 * (re[uu] + re[ll])
    w1 = 0.5 * (im[ul] + im[lu])
    w2 = 0.5 * (re[ul] - re[lu])
    w3 = 0.5 * (im[uu] - im[ll])
    vec_sq = w1 * w1 + w2 * w2 + w3 * w3
    w0_sq = w0 * w0
    inv = 1.0 / jnp.maximum(w0_sq + vec_sq, 0.5)
    scale = -2.0 * w0 * inv
    r0, r1, r2, r3 = (w0_sq - vec_sq) * inv, scale * w1, scale * w2, scale * w3
    x0, x1, x2, x3 = turn
    return (
        x0 * r0 - (x1 * r1 + x2 * r2 + x3 * r3),
        x0 * r1 + r0 * x1 - (x2 * r3 - x3 * r2),
        x0 * r2 + r0 * x2 - (x3 * r1 - x1 * r3),
        x0 * r3 + r0 * x3 - (x1 * r2 - x2 * r1),
    )


def closed(six):
    re, im = list(six[0]), list(six[1])
    for col in range(3):
        a, b = (col + 1) % 3, (col + 2) % 3
        real = (re[a] * re[3 + b] - im[a] * im[3 + b]) - (re[b] * re[3 + a] - im[b] * im[3 + a])
        imag = (re[a] * im[3 + b] + im[a] * re[3 + b]) - (re[b] * im[3 + a] + im[b] * re[3 + a])
        re.append(real)
        im.append(-imag)
    return re, im


def turn_lanes(value, steps):
    return pltpu.roll(value, (-steps) % LANES, 1)


def turn_rows(value, steps):
    return pltpu.roll(value, (-steps) % 8, 0)


class Shifts:
    def __init__(self):
        lane = lax.broadcasted_iota(jnp.int32, (8, LANES), 1)
        row = lax.broadcasted_iota(jnp.int32, (8, LANES), 0)
        self.depth = lane % LZ
        self.lane = lane
        self.slot = row % 4
        self.odd = ((lane // LZ + lane) % 2) == 1
        self.low_rows = row < 4
        self.even_lane = lane % 2 == 0

    def rows(self, value, offset):
        if offset > 0:
            turned = turn_lanes(value, LZ)
            after = jnp.where(self.slot == 2, turn_rows(turned, -2), turn_rows(turned, 1))
            return jnp.where(self.lane < LANES - LZ, turned, after)
        turned = turn_lanes(value, -LZ)
        before = jnp.where(self.slot == 0, turn_rows(turned, 2), turn_rows(turned, -1))
        return jnp.where(self.lane >= LZ, turned, before)

    def deep(self, value, offset):
        if offset > 0:
            return jnp.where(
                self.depth < LZ - offset, turn_lanes(value, offset), turn_lanes(value, offset - LZ)
            )
        return jnp.where(
            self.depth >= -offset, turn_lanes(value, offset), turn_lanes(value, LZ + offset)
        )

    def pair_swap(self, value):
        return jnp.where(self.even_lane, turn_lanes(value, 1), turn_lanes(value, -1))


def kernel(
    time_hbm, space_hbm, turn_hbm, out_hbm, log_hbm,
    time_raw, space_raw, turn_raw, left_out, left_in, left_next,
    field, bonds, shifted, pack_out, pack_in, loop_rows, loop_out, loop_in,
    oper, chain_a, chain_b, group, part, final,
    in_sem, edge_out, edge_in, halo_out, halo_in, loop_sent, loop_got, local_sem, back_sem, done_sem,
):
    ix, iz, ia = lax.axis_index("ta_0"), lax.axis_index("ta_1"), lax.axis_index("sa")
    nx, nz, na = 4, 4, lax.axis_size("sa")
    left, right = lax.rem(ia + na - 1, na), lax.rem(ia + 1, na)
    slab = ix * nz + iz
    earlier = lax.rem(slab + nx * nz - 1, nx * nz)
    later = lax.rem(slab + 1, nx * nz)
    earlier_x, earlier_z = earlier // nz, lax.rem(earlier, nz)
    later_x, later_z = later // nz, lax.rem(later, nz)
    halves = 2 * SWEEPS

    for t in range(4):
        for j in range(3):
            lanes, rows = pl.ds(LANES * j, LANES), pl.ds(8 * t + 2 * j, 2)
            pltpu.make_async_copy(
                time_hbm.at[:, t, :, lanes], time_raw.at[:, rows, :], in_sem.at[0]).start()
            pltpu.make_async_copy(
                space_hbm.at[:, :, t, :, lanes], space_raw.at[:, :, rows, :], in_sem.at[1]).start()
    for t in range(4):
        for j in range(3):
            lanes, rows = pl.ds(LANES * j, LANES), pl.ds(8 * t + 2 * j, 2)
            pltpu.make_async_copy(
                turn_hbm.at[:, :, :, t, :, lanes], turn_raw.at[:, :, :, rows, :], in_sem.at[2]
            ).start()

    barrier = pltpu.get_barrier_semaphore()
    peers = []
    for step in range(1, nx * nz):
        peer = lax.rem(slab + step, nx * nz)
        peers.append((peer // nz, lax.rem(peer, nz), ia))
    peers += [(ix, iz, left), (ix, iz, right)]
    peers += [(earlier_x, earlier_z, right), (later_x, later_z, left)]
    for peer in peers:
        pl.semaphore_signal(barrier, inc=1, device_id=peer, device_id_type=MESH)

    def remote(src, dst, out_sem, got_sem, target):
        return pltpu.make_async_remote_copy(
            src_ref=src, dst_ref=dst, send_sem=out_sem, recv_sem=got_sem,
            device_id=target, device_id_type=MESH)

    def landed(ref, sem):
        pltpu.make_async_copy(ref, ref, sem).wait()

    shifts = Shifts()
    odd = shifts.odd

    def own(parity, first, second):
        return jnp.where(odd, first, second) if parity else jnp.where(odd, second, first)

    def split(values):
        return values[:9], values[9:]

    def pack(number, block, parity, links):
        for k in range(9):
            real, partner = links[0][k], shifts.pair_swap(links[1][k])
            pack_out[number, block, 0, k] = own(parity, real, partner)
            pack_out[number, block, 1, k] = own(parity, partner, real)

    def halo(number, block, side, target):
        return remote(
            pack_out.at[number, block, side], pack_in.at[number, block, side],
            halo_out.at[number, block, side], halo_in.at[number, block, side], (ix, iz, target))

    landed(time_raw.at[:, pl.ds(0, 24), :], in_sem.at[0])
    for block in range(2):
        packed = []
        for entry in range(18):
            first = time_raw[entry, pl.ds(16 * block, 8, stride=2), :]
            second = time_raw[entry, pl.ds(16 * block + 1, 8, stride=2), :]
            field[0, entry, pl.ds(8 * block, 8), :] = own(0, first, second)
            value = own(1, first, second)
            field[1, entry, pl.ds(8 * block, 8), :] = value
            packed.append(value)
        pack(0, block, 1, split(packed))
    landed(space_raw.at[:, :, pl.ds(0, 24), :], in_sem.at[1])
    two_rows = [*range(6), *range(9, 15)]
    for block in range(2):
        for place, entry in enumerate(two_rows):
            left_out[place, pl.ds(8 * block, 8), :] = (
                space_raw[0, entry, pl.ds(16 * block + 1, 8, stride=2), :])

    def raw(direction, at, column):
        return [space_raw[direction, k, pl.ds(at + column, 8, stride=2), :] for k in range(18)]

    def inner_bonds(block):
        at, to = 16 * block, pl.ds(8 * block, 8)
        if not isinstance(block, int):
            at, to = pl.multiple_of(at, 16), pl.ds(pl.multiple_of(8 * block, 8), 8)

        def put(parity, place, matrix):
            for k in range(9):
                bonds[parity, place, k, to, :] = matrix[0][k]
                bonds[parity, place, 9 + k, to, :] = matrix[1][k]

        inner = raw(0, at, 0)
        inner_dag = dagger(split(inner))
        inner_dag = inner_dag[0] + inner_dag[1]
        for parity in (0, 1):
            put(parity, 0, split([own(parity, a, b) for a, b in zip(inner, inner_dag)]))
        for direction, shift in ((1, shifts.rows), (2, shifts.deep)):
            first, second = raw(direction, at, 0), raw(direction, at, 1)
            for parity in (0, 1):
                here = [own(parity, a, b) for a, b in zip(first, second)]
                put(parity, 2 * direction - 1, split(here))
                back = [shift(value, -1) for value in here]
                put(1 - parity, 2 * direction, dagger(split(back)))

    def outer_bonds(block):
        to = pl.ds(8 * block, 8)
        outer = raw(0, 16 * block, 1)
        if block < 2:
            six = [left_in[k, to, :] for k in range(12)]
        else:
            six = [left_next[k, pl.ds(1, 8, stride=2), :] for k in range(12)]
        beyond = dagger(closed((six[:6], six[6:])))
        beyond = beyond[0] + beyond[1]
        for parity in (0, 1):
            for k in range(18):
                bonds[parity, 5, k, to, :] = own(parity, beyond[k], outer[k])

    @pl.loop(0, 2)
    def _(block):
        inner_bonds(block)

    pl.semaphore_wait(barrier, len(peers))
    for block in range(2):
        for side, target in ((0, left), (1, right)):
            halo(0, block, side, target).start()
    edges = [remote(left_out, left_in, edge_out.at[0], edge_in.at[0], (ix, iz, right))]
    for half in range(2):
        rows = pl.ds(0, 6)
        edges.append(remote(
            space_raw.at[:, pl.ds(9 * half, 6), rows, :],
            space_raw.at[:, pl.ds(9 * half, 6), pl.ds(32, 6), :],
            edge_out.at[1 + half], edge_in.at[1 + half], (earlier_x, earlier_z, ia)))
        edges.append(remote(
            space_raw.at[0, pl.ds(9 * half, 6), rows, :],
            left_next.at[pl.ds(6 * half, 6), rows, :],
            edge_out.at[3 + half], edge_in.at[3 + half], (earlier_x, earlier_z, right)))
    for copy in edges:
        copy.start()
    landed(turn_raw.at[:, :, :, pl.ds(0, 24), :], in_sem.at[2])
    edges[0].wait_recv()
    for block in range(2):
        outer_bonds(block)

    def half_sweep(sweep, parity):
        number = 2 * sweep + parity

        @pl.loop(0, 2)
        def _(block):
            rows = pl.ds(pl.multiple_of(8 * block, 8), 8)
            rows_later = pl.ds(8 * block + 4, 8)

            if parity == 0:
                @pl.when(jnp.logical_and(sweep == 0, block == 1))
                def _():
                    for copy in edges[1:]:
                        copy.wait_recv()
                    for direction in range(3):
                        six = [space_raw[direction, k, pl.ds(32, 8), :] for k in two_rows]
                        re, im = closed((six[:6], six[6:]))
                        for k in range(6, 9):
                            space_raw[direction, k, pl.ds(32, 8), :] = re[k]
                            space_raw[direction, 9 + k, pl.ds(32, 8), :] = im[k]
                    inner_bonds(2)
                    outer_bonds(2)

            def load(ref, lead, where):
                return split([ref[(*lead, k, where, slice(None))] for k in range(18)])

            for entry in range(18):
                value = field[1 - parity, entry, rows, :]
                shifted[0, entry] = shifts.rows(value, 1)
                shifted[1, entry] = shifts.rows(value, -1)
                shifted[2, entry] = shifts.deep(value, 1)
                shifted[3, entry] = shifts.deep(value, -1)
            total = ([None] * 9, [None] * 9)
            total = staple_term(
                total, load(bonds, (parity, 0), rows_later), load(bonds, (parity, 0), rows),
                load(field, (1 - parity,), rows))
            for place in range(1, 5):
                total = staple_term(
                    total, load(bonds, (parity, place), rows_later),
                    load(bonds, (parity, place), rows),
                    load(shifted, (place - 1,), slice(None)))

            for side in range(2):
                halo(number, block, side, left).wait_recv()
            beyond_re, beyond_im = [], []
            for k in range(9):
                from_left = pack_in[number, block, 1, k]
                from_right = pack_in[number, block, 0, k]
                beyond_re.append(own(parity, from_left, from_right))
                beyond_im.append(shifts.pair_swap(own(parity, from_right, from_left)))
            total = staple_term(
                total, load(bonds, (parity, 5), rows_later), load(bonds, (parity, 5), rows),
                (beyond_re, beyond_im))
            links = load(field, (parity,), rows)
            product = times(links, total)
            for plane, (upper, lower) in enumerate(PLANES):
                base = pl.multiple_of(16 * block, 16)
                turn = [
                    own(parity, turn_raw[sweep, plane, k, pl.ds(base, 8, stride=2), :],
                        turn_raw[sweep, plane, k, pl.ds(base + 1, 8, stride=2), :])
                    for k in range(4)]
                quat = reflected(product, upper, lower, turn)
                links = rotate_rows(links, upper, lower, quat)
                if plane < 2:
                    product = rotate_rows(product, upper, lower, quat)
            for k in range(9):
                field[parity, k, rows, :] = links[0][k]
                field[parity, 9 + k, rows, :] = links[1][k]

            @pl.when(number < halves - 1)
            def _():
                pack(number + 1, block, parity, links)
                for side, target in ((0, left), (1, right)):
                    halo(number + 1, block, side, target).start()

    def send_loops(sweep, parity):
        low = shifts.low_rows
        number = 2 * sweep + parity
        even, uneven = [], []
        for entry in range(18):
            a = field[parity, entry, pl.ds(0, 8), :]
            b = field[parity, entry, pl.ds(4, 8), :]
            c = field[parity, entry, pl.ds(8, 8), :]
            even.append(jnp.where(low, a, b))
            uneven.append(jnp.where(low, b, c))
        re, im = times(split(even), split(uneven))
        re, im = times((re, im), ([turn_rows(v, 4) for v in re], [turn_rows(v, 4) for v in im]))
        for entry, value in enumerate(re + im):
            loop_rows[pl.ds(8 * entry, 8), :] = value
        for j in range(3):
            for third in range(3):
                loop_out[number, j, pl.ds(8 * third, 8), :] = (
                    loop_rows[pl.ds(64 * third + j, 8, stride=8), :])

        def loop_to(peer_x):
            at = pl.multiple_of(24 * (2 * ix + parity), 8)
            return (
                loop_out.at[number, peer_x - 1, pl.ds(0, 18), :],
                loop_in.at[sweep, iz, pl.ds(at, 18), :])

        for step in range(nx * nz):
            if step == 0:
                @pl.when(ix > 0)
                def _():
                    pltpu.make_async_copy(*loop_to(ix), local_sem.at[number]).start()
            else:
                peer = lax.rem(slab + step, nx * nz)
                peer_x, peer_z = peer // nz, lax.rem(peer, nz)

                @pl.when(peer_x > 0)
                def _():
                    remote(
                        *loop_to(peer_x), loop_sent.at[number], loop_got.at[number],
                        (peer_x, peer_z, ia)).start()

    @pl.loop(0, SWEEPS)
    def _(sweep):
        for parity in (0, 1):
            half_sweep(sweep, parity)
            send_loops(sweep, parity)

    def normalized(load, store, log):
        square = None
        for k in range(162):
            value = load(k)
            square = value * value if square is None else square + value * value
        rms = jnp.sqrt(square / 162.0 + 1e-06)
        inv = 1.0 / rms
        for k in range(162):
            store(k, load(k) * inv)
        return log + jnp.log(rms)

    def combine(left_ref, right_ref, dst_ref, keep):
        @pl.loop(0, 9)
        def _(row):
            for half in range(3):
                columns = range(3 * half, 3 * half + 3)
                re, im = [None] * 3, [None] * 3
                for mid in range(9):
                    a_re, a_im = left_ref[9 * row + mid], left_ref[81 + 9 * row + mid]
                    for place, col in enumerate(columns):
                        b_re, b_im = right_ref[9 * mid + col], right_ref[81 + 9 * mid + col]
                        p_re = a_re * b_re - a_im * b_im
                        p_im = a_re * b_im + a_im * b_re
                        re[place] = p_re if re[place] is None else re[place] + p_re
                        im[place] = p_im if im[place] is None else im[place] + p_im
                for place, col in enumerate(columns):
                    dst_ref[9 * row + col] = re[place]
                    dst_ref[81 + 9 * row + col] = im[place]
        log = normalized(
            lambda k: dst_ref[k], lambda k, value: dst_ref.__setitem__(k, keep(k, value)),
            left_ref[162] + right_ref[162])
        dst_ref[162] = keep(162, log)

    def result_to(target):
        lanes = pl.ds(pl.multiple_of(LANES * (ix - 1), LANES), LANES)
        rows = pl.ds(2 * target, 2)
        return (
            (final.at[pl.ds(0, 162), rows, :], out_hbm.at[:, :, lanes]),
            (final.at[162, rows, :], log_hbm.at[:, lanes]))

    @pl.when(ix > 0)
    def _():
        for number in range(halves):
            ref = loop_out.at[number, 0, pl.ds(0, 18), :]
            landed(ref, local_sem.at[number])
            landed(space_raw.at[0, :, pl.ds(0, 15), :], loop_got.at[number])

        @pl.loop(0, nz)
        def _(slot):
            for sweep in range(SWEEPS):
                loops = [loop_in[sweep, slot, pl.ds(k, 8, stride=24), :] for k in range(18)]
                partner = [shifts.deep(value, 4) for value in loops]
                for a in range(3):
                    for c in range(3):
                        for e in range(3):
                            for d in range(3):
                                l_re, l_im = loops[3 * a + e], loops[9 + 3 * a + e]
                                r_re, r_im = partner[3 * c + d], partner[9 + 3 * c + d]
                                re = l_re * r_re + l_im * r_im
                                im = l_im * r_re - l_re * r_im
                                at = 9 * (3 * a + c) + 3 * e + d
                                if sweep:
                                    re = oper[slot, at] + re
                                    im = oper[slot, 81 + at] + im
                                oper[slot, at] = re
                                oper[slot, 81 + at] = im
            third = 1.0 / SWEEPS
            log = normalized(
                lambda k: oper[slot, k] * third,
                lambda k, value: oper.at[slot].__setitem__(k, value), jnp.zeros((8, LANES)))
            oper[slot, 162] = log

        @pl.loop(0, 163)
        def _(k):
            part[0, k] = oper[0, k]

        @pl.loop(1, nz)
        def _(slot):
            combine(part.at[slot - 1], oper.at[slot], part.at[slot], lambda k, value: value)

        row = lax.broadcasted_iota(jnp.int32, (8, LANES), 0)

        def moved(value, k, rows):
            unit = 1.0 if k < 81 and k % 10 == 0 else 0.0
            return jnp.where(row < rows, unit, turn_rows(value, -rows))

        def by_column(k, value):
            swapped = jnp.where(row % 2 == 0, turn_rows(value, 1), turn_rows(value, -1))
            return jnp.where(odd, swapped, value)

        for k in range(163):
            chain_a[k] = moved(part[nz - 1, k], k, 2)
            chain_b[k] = moved(chain_a[k], k, 2)
        combine(chain_b, chain_a, group, lambda k, value: jnp.where(row < 2, chain_a[k], value))
        for k in range(163):
            chain_b[k] = moved(group[k], k, 4)
        combine(chain_b, group, chain_a, lambda k, value: jnp.where(row < 4, group[k], value))
        combine(chain_a, part.at[iz], final, by_column)

        for target in range(nx):
            @pl.when(ix == target)
            def _():
                for piece, (src, dst) in enumerate(result_to(target)):
                    pltpu.make_async_copy(src, dst, done_sem.at[piece]).start()

            @pl.when(ix != target)
            def _():
                for piece, (src, dst) in enumerate(result_to(target)):
                    remote(
                        src, dst, done_sem.at[2 + piece], back_sem.at[piece, ix], (target, iz, ia)
                    ).start()
        for piece, (src, dst) in enumerate(result_to(0)):
            pltpu.make_async_copy(src, dst, done_sem.at[piece]).wait()

    for source in range(1, nx):
        @pl.when(ix != source)
        def _():
            landed(final.at[pl.ds(0, 162), pl.ds(0, 2), :], back_sem.at[0, source])
            landed(final.at[162, pl.ds(0, 2), :], back_sem.at[1, source])

    for copy in edges:
        copy.wait_send()
    for number in range(halves):
        for block in range(2):
            for side in range(2):
                halo(number, block, side, left).wait_send()

    @pl.when(ix == 0)
    def _():
        for number in range(halves):
            landed(space_raw.at[0, :, pl.ds(0, 12), :], loop_sent.at[number])

    @pl.when(ix > 0)
    def _():
        for number in range(halves):
            landed(space_raw.at[0, :, pl.ds(0, 11), :], loop_sent.at[number])
        landed(final.at[pl.ds(0, 162), pl.ds(0, 6), :], done_sem.at[2])
        landed(final.at[162, pl.ds(0, 6), :], done_sem.at[3])


def per_device(temporal_links, spatial_links, rotations):
    f32, dma = jnp.float32, pltpu.SemaphoreType.DMA
    halves = 2 * SWEEPS
    transfer, log_scale = pl.pallas_call(
        kernel,
        name="slab_chain",
        out_shape=(
            jax.ShapeDtypeStruct((162, 2, 3 * LANES), f32),
            jax.ShapeDtypeStruct((2, 3 * LANES), f32),
        ),
        in_specs=[pl.BlockSpec(memory_space=pl.ANY)] * 3,
        out_specs=[pl.BlockSpec(memory_space=pl.ANY)] * 2,
        scratch_shapes=[
            pltpu.VMEM((18, 32, LANES), f32),
            pltpu.VMEM((3, 18, 48, LANES), f32),
            pltpu.VMEM((3, 3, 4, 32, LANES), f32),
            pltpu.VMEM((12, 16, LANES), f32),
            pltpu.VMEM((12, 16, LANES), f32),
            pltpu.VMEM((12, 16, LANES), f32),
            pltpu.VMEM((2, 18, 16, LANES), f32),
            pltpu.VMEM((2, 6, 18, 24, LANES), f32),
            pltpu.VMEM((4, 18, 8, LANES), f32),
            pltpu.VMEM((halves, 2, 2, 9, 8, LANES), f32),
            pltpu.VMEM((halves, 2, 2, 9, 8, LANES), f32),
            pltpu.VMEM((192, LANES), f32),
            pltpu.VMEM((halves, 3, 24, LANES), f32),
            pltpu.VMEM((SWEEPS, 4, 192, LANES), f32),
            pltpu.VMEM((4, 163, 8, LANES), f32),
            pltpu.VMEM((163, 8, LANES), f32),
            pltpu.VMEM((163, 8, LANES), f32),
            pltpu.VMEM((163, 8, LANES), f32),
            pltpu.VMEM((4, 163, 8, LANES), f32),
            pltpu.VMEM((163, 8, LANES), f32),
            dma((3,)), dma((5,)), dma((5,)), dma((halves, 2, 2)), dma((halves, 2, 2)),
            dma((halves,)), dma((halves,)), dma((halves,)), dma((2, 4)), dma((4,)),
        ],
        compiler_params=pltpu.CompilerParams(collective_id=0, has_side_effects=True),
    )(temporal_links, spatial_links, rotations)
    return transfer.reshape(2, 9, 9, 1, 2, 3 * LANES), log_scale.reshape(1, 2, 3 * LANES)


def solution(mesh):
    split = Mesh(mesh.devices.reshape(4, 4, mesh.shape["sa"]), AXES)
    slabs = ("ta_0", "ta_1")
    return jax.shard_map(
        per_device,
        mesh=split,
        in_specs=(
            P(None, slabs, "sa", None),
            P(None, None, slabs, "sa", None),
            P(None, None, None, slabs, "sa", None),
        ),
        out_specs=(P(None, None, None, slabs, "sa", None), P(slabs, "sa", None)),
        check_vma=False,
    )
```

```python
import jax
import jax.numpy as jnp
from jax import lax
from jax.experimental import pallas as pl
from jax.experimental.pallas import tpu as pltpu
from jax.sharding import Mesh
from jax.sharding import PartitionSpec as P

SWEEPS = 3
LZ = 16
LANES = 128
MESH = pl.DeviceIdType.MESH
AXES = ("ta_0", "ta_1", "sa")
PLANES = ((0, 1), (1, 2), (0, 2))


def times(left, right):
    out_re, out_im = [], []
    for row in range(3):
        for col in range(3):
            re = im = None
            for mid in range(3):
                a_re, a_im = left[0][3 * row + mid], left[1][3 * row + mid]
                b_re, b_im = right[0][3 * mid + col], right[1][3 * mid + col]
                p_re = a_re * b_re - a_im * b_im
                p_im = a_re * b_im + a_im * b_re
                re = p_re if re is None else re + p_re
                im = p_im if im is None else im + p_im
            out_re.append(re)
            out_im.append(im)
    return out_re, out_im


def staple_term(total, later, now, link):
    total_re, total_im = list(total[0]), list(total[1])
    for col in range(3):
        mid_re, mid_im = [], []
        for k in range(3):
            re = im = None
            for m in range(3):
                a_re, a_im = now[0][3 * col + m], now[1][3 * col + m]
                b_re, b_im = link[0][3 * m + k], link[1][3 * m + k]
                p_re = a_re * b_re - a_im * b_im
                p_im = a_re * b_im + a_im * b_re
                re = p_re if re is None else re + p_re
                im = p_im if im is None else im + p_im
            mid_re.append(re)
            mid_im.append(im)
        for row in range(3):
            re, im = total_re[3 * row + col], total_im[3 * row + col]
            for k in range(3):
                a_re, a_im = later[0][3 * row + k], later[1][3 * row + k]
                p_re = a_re * mid_re[k] + a_im * mid_im[k]
                p_im = a_im * mid_re[k] - a_re * mid_im[k]
                re = p_re if re is None else re + p_re
                im = p_im if im is None else im + p_im
            total_re[3 * row + col], total_im[3 * row + col] = re, im
    return total_re, total_im


def dagger(matrix):
    order = (0, 3, 6, 1, 4, 7, 2, 5, 8)
    return [matrix[0][k] for k in order], [-matrix[1][k] for k in order]


def rotate_rows(matrix, upper, lower, quat):
    q0, q1, q2, q3 = quat
    re, im = list(matrix[0]), list(matrix[1])
    for col in range(3):
        u_re, u_im = matrix[0][3 * upper + col], matrix[1][3 * upper + col]
        l_re, l_im = matrix[0][3 * lower + col], matrix[1][3 * lower + col]
        re[3 * upper + col] = q0 * u_re - q3 * u_im + q2 * l_re - q1 * l_im
        im[3 * upper + col] = q0 * u_im + q3 * u_re + q2 * l_im + q1 * l_re
        re[3 * lower + col] = q0 * l_re + q3 * l_im - q2 * u_re - q1 * u_im
        im[3 * lower + col] = q0 * l_im - q3 * l_re - q2 * u_im + q1 * u_re
    return re, im


def reflected(product, upper, lower, turn):
    re, im = product
    uu, ul, lu, ll = 4 * upper, 3 * upper + lower, 3 * lower + upper, 4 * lower
    w0 = 0.5 * (re[uu] + re[ll])
    w1 = 0.5 * (im[ul] + im[lu])
    w2 = 0.5 * (re[ul] - re[lu])
    w3 = 0.5 * (im[uu] - im[ll])
    vec_sq = w1 * w1 + w2 * w2 + w3 * w3
    w0_sq = w0 * w0
    inv = 1.0 / jnp.maximum(w0_sq + vec_sq, 0.5)
    scale = -2.0 * w0 * inv
    r0, r1, r2, r3 = (w0_sq - vec_sq) * inv, scale * w1, scale * w2, scale * w3
    x0, x1, x2, x3 = turn
    return (
        x0 * r0 - (x1 * r1 + x2 * r2 + x3 * r3),
        x0 * r1 + r0 * x1 - (x2 * r3 - x3 * r2),
        x0 * r2 + r0 * x2 - (x3 * r1 - x1 * r3),
        x0 * r3 + r0 * x3 - (x1 * r2 - x2 * r1),
    )


def closed(six):
    re, im = list(six[0]), list(six[1])
    for col in range(3):
        a, b = (col + 1) % 3, (col + 2) % 3
        real = (re[a] * re[3 + b] - im[a] * im[3 + b]) - (re[b] * re[3 + a] - im[b] * im[3 + a])
        imag = (re[a] * im[3 + b] + im[a] * re[3 + b]) - (re[b] * im[3 + a] + im[b] * re[3 + a])
        re.append(real)
        im.append(-imag)
    return re, im


def turn_lanes(value, steps):
    return pltpu.roll(value, (-steps) % LANES, 1)


def turn_rows(value, steps):
    return pltpu.roll(value, (-steps) % 8, 0)


class Shifts:
    def __init__(self):
        lane = lax.broadcasted_iota(jnp.int32, (8, LANES), 1)
        row = lax.broadcasted_iota(jnp.int32, (8, LANES), 0)
        self.depth = lane % LZ
        self.lane = lane
        self.slot = row % 4
        self.odd = ((lane // LZ + lane) % 2) == 1
        self.low_rows = row < 4
        self.even_lane = lane % 2 == 0

    def rows(self, value, offset):
        if offset > 0:
            turned = turn_lanes(value, LZ)
            after = jnp.where(self.slot == 2, turn_rows(turned, -2), turn_rows(turned, 1))
            return jnp.where(self.lane < LANES - LZ, turned, after)
        turned = turn_lanes(value, -LZ)
        before = jnp.where(self.slot == 0, turn_rows(turned, 2), turn_rows(turned, -1))
        return jnp.where(self.lane >= LZ, turned, before)

    def deep(self, value, offset):
        if offset > 0:
            return jnp.where(
                self.depth < LZ - offset, turn_lanes(value, offset), turn_lanes(value, offset - LZ)
            )
        return jnp.where(
            self.depth >= -offset, turn_lanes(value, offset), turn_lanes(value, LZ + offset)
        )

    def pair_swap(self, value):
        return jnp.where(self.even_lane, turn_lanes(value, 1), turn_lanes(value, -1))


def kernel(
    time_hbm, space_hbm, turn_hbm, out_hbm, log_hbm,
    time_raw, space_raw, turn_raw, left_out, left_in, left_next,
    field, bonds, shifted, pack_out, pack_in, loop_rows, loop_out, loop_in,
    oper, chain_a, chain_b, group, sums, final,
    in_sem, edge_out, edge_in, halo_out, halo_in, loop_sent, loop_got, local_sem, back_sem, done_sem,
):
    ix, iz, ia = lax.axis_index("ta_0"), lax.axis_index("ta_1"), lax.axis_index("sa")
    nx, nz, na = 4, 4, lax.axis_size("sa")
    left, right = lax.rem(ia + na - 1, na), lax.rem(ia + 1, na)
    slab = ix * nz + iz
    earlier = lax.rem(slab + nx * nz - 1, nx * nz)
    later = lax.rem(slab + 1, nx * nz)
    earlier_x, earlier_z = earlier // nz, lax.rem(earlier, nz)
    later_x, later_z = later // nz, lax.rem(later, nz)
    halves = 2 * SWEEPS

    for t in range(4):
        for j in range(3):
            lanes, rows = pl.ds(LANES * j, LANES), pl.ds(8 * t + 2 * j, 2)
            pltpu.make_async_copy(
                time_hbm.at[:, t, :, lanes], time_raw.at[:, rows, :], in_sem.at[0]).start()
            pltpu.make_async_copy(
                space_hbm.at[:, :, t, :, lanes], space_raw.at[:, :, rows, :], in_sem.at[1]).start()
    for t in range(4):
        for j in range(3):
            lanes, rows = pl.ds(LANES * j, LANES), pl.ds(8 * t + 2 * j, 2)
            pltpu.make_async_copy(
                turn_hbm.at[:, :, :, t, :, lanes], turn_raw.at[:, :, :, rows, :], in_sem.at[2]
            ).start()

    barrier = pltpu.get_barrier_semaphore()
    peers = []
    for step in range(1, nx * nz):
        peer = lax.rem(slab + step, nx * nz)
        peers.append((peer // nz, lax.rem(peer, nz), ia))
    peers += [(ix, iz, left), (ix, iz, right)]
    peers += [(earlier_x, earlier_z, right), (later_x, later_z, left)]
    for peer in peers:
        pl.semaphore_signal(barrier, inc=1, device_id=peer, device_id_type=MESH)

    def remote(src, dst, out_sem, got_sem, target):
        return pltpu.make_async_remote_copy(
            src_ref=src, dst_ref=dst, send_sem=out_sem, recv_sem=got_sem,
            device_id=target, device_id_type=MESH)

    def landed(ref, sem):
        pltpu.make_async_copy(ref, ref, sem).wait()

    shifts = Shifts()
    odd = shifts.odd

    def own(parity, first, second):
        return jnp.where(odd, first, second) if parity else jnp.where(odd, second, first)

    def split(values):
        return values[:9], values[9:]

    def pack(number, block, parity, links):
        for k in range(9):
            real, partner = links[0][k], shifts.pair_swap(links[1][k])
            pack_out[number, block, 0, k] = own(parity, real, partner)
            pack_out[number, block, 1, k] = own(parity, partner, real)

    def send_halo(number, block, side, target):
        for at in (0, 4):
            rows = pl.ds(at, 3)
            remote(
                pack_out.at[number, block, side, :, rows, :],
                pack_in.at[number, block, side, :, rows, :],
                halo_out.at[number, block, side], halo_in.at[number, block, side],
                (ix, iz, target)).start()

    def await_halo(sem, number, block, side):
        landed(pack_in.at[number, block, side, :, pl.ds(0, 6), :], sem.at[number, block, side])

    two_rows = [*range(6), *range(9, 15)]
    landed(space_raw.at[:, :, pl.ds(0, 24), :], in_sem.at[1])
    for block in range(2):
        for place, entry in enumerate(two_rows):
            left_out[place, pl.ds(8 * block, 8), :] = (
                space_raw[0, entry, pl.ds(16 * block + 1, 8, stride=2), :])
    landed(time_raw.at[:, pl.ds(0, 24), :], in_sem.at[0])
    for block in range(2):
        packed = []
        for entry in range(18):
            first = time_raw[entry, pl.ds(16 * block, 8, stride=2), :]
            second = time_raw[entry, pl.ds(16 * block + 1, 8, stride=2), :]
            field[0, entry, pl.ds(8 * block, 8), :] = own(0, first, second)
            value = own(1, first, second)
            field[1, entry, pl.ds(8 * block, 8), :] = value
            packed.append(value)
        pack(0, block, 1, split(packed))
    pl.semaphore_wait(barrier, len(peers))
    for block in range(2):
        for side, target in ((0, left), (1, right)):
            send_halo(0, block, side, target)
    edges = []
    for t in range(4):
        rows = pl.ds(4 * t, 3)
        edges.append(remote(
            left_out.at[:, rows, :], left_in.at[:, rows, :], edge_out.at[0], edge_in.at[0],
            (ix, iz, right)))
    for half in range(2):
        rows = pl.ds(0, 6)
        edges.append(remote(
            space_raw.at[:, pl.ds(9 * half, 6), rows, :],
            space_raw.at[:, pl.ds(9 * half, 6), pl.ds(32, 6), :],
            edge_out.at[1 + half], edge_in.at[1 + half], (earlier_x, earlier_z, ia)))
    edges.append(remote(
        left_out.at[:, pl.ds(0, 3), :], left_next.at[:, pl.ds(0, 3), :],
        edge_out.at[3], edge_in.at[3], (earlier_x, earlier_z, right)))
    for copy in edges:
        copy.start()
    covers = (
        left_in.at[:, pl.ds(0, 12), :], space_raw.at[:, pl.ds(0, 6), pl.ds(0, 6), :],
        space_raw.at[:, pl.ds(0, 6), pl.ds(0, 6), :], left_in.at[:, pl.ds(0, 3), :])

    def raw(direction, at, column):
        return [space_raw[direction, k, pl.ds(at + column, 8, stride=2), :] for k in range(18)]

    def inner_bonds(block):
        at, to = 16 * block, pl.ds(8 * block, 8)
        if not isinstance(block, int):
            at, to = pl.multiple_of(at, 16), pl.ds(pl.multiple_of(8 * block, 8), 8)

        def put(parity, place, matrix):
            for k in range(9):
                bonds[parity, place, k, to, :] = matrix[0][k]
                bonds[parity, place, 9 + k, to, :] = matrix[1][k]

        inner = raw(0, at, 0)
        inner_dag = dagger(split(inner))
        inner_dag = inner_dag[0] + inner_dag[1]
        for parity in (0, 1):
            put(parity, 0, split([own(parity, a, b) for a, b in zip(inner, inner_dag)]))
        for direction, shift in ((1, shifts.rows), (2, shifts.deep)):
            first, second = raw(direction, at, 0), raw(direction, at, 1)
            for parity in (0, 1):
                here = [own(parity, a, b) for a, b in zip(first, second)]
                put(parity, 2 * direction - 1, split(here))
                back = [shift(value, -1) for value in here]
                put(1 - parity, 2 * direction, dagger(split(back)))

    def outer_bonds(block):
        to = pl.ds(8 * block, 8)
        outer = raw(0, 16 * block, 1)
        if block < 2:
            six = [left_in[k, to, :] for k in range(12)]
        else:
            six = [left_next[k] for k in range(12)]
        beyond = dagger(closed((six[:6], six[6:])))
        beyond = beyond[0] + beyond[1]
        for parity in (0, 1):
            for k in range(18):
                bonds[parity, 5, k, to, :] = own(parity, beyond[k], outer[k])

    @pl.loop(0, 2)
    def _(block):
        inner_bonds(block)

    landed(turn_raw.at[:, :, :, pl.ds(0, 24), :], in_sem.at[2])
    landed(covers[0], edge_in.at[0])
    for block in range(2):
        outer_bonds(block)

    def half_sweep(sweep, parity):
        number = 2 * sweep + parity

        @pl.loop(0, 2)
        def _(block):
            rows = pl.ds(pl.multiple_of(8 * block, 8), 8)
            rows_later = pl.ds(8 * block + 4, 8)

            if parity == 0:
                @pl.when(jnp.logical_and(sweep == 0, block == 1))
                def _():
                    for piece in range(1, 4):
                        landed(covers[piece], edge_in.at[piece])
                    for direction in range(3):
                        six = [space_raw[direction, k, pl.ds(32, 8), :] for k in two_rows]
                        re, im = closed((six[:6], six[6:]))
                        for k in range(6, 9):
                            space_raw[direction, k, pl.ds(32, 8), :] = re[k]
                            space_raw[direction, 9 + k, pl.ds(32, 8), :] = im[k]
                    inner_bonds(2)
                    outer_bonds(2)

            def load(ref, lead, where):
                return split([ref[(*lead, k, where, slice(None))] for k in range(18)])

            for entry in range(18):
                value = field[1 - parity, entry, rows, :]
                shifted[0, entry] = shifts.rows(value, 1)
                shifted[1, entry] = shifts.rows(value, -1)
                shifted[2, entry] = shifts.deep(value, 1)
                shifted[3, entry] = shifts.deep(value, -1)
            total = ([None] * 9, [None] * 9)
            total = staple_term(
                total, load(bonds, (parity, 0), rows_later), load(bonds, (parity, 0), rows),
                load(field, (1 - parity,), rows))
            for place in range(1, 5):
                total = staple_term(
                    total, load(bonds, (parity, place), rows_later),
                    load(bonds, (parity, place), rows),
                    load(shifted, (place - 1,), slice(None)))

            for side in range(2):
                await_halo(halo_in, number, block, side)
            beyond_re, beyond_im = [], []
            for k in range(9):
                from_left = pack_in[number, block, 1, k]
                from_right = pack_in[number, block, 0, k]
                beyond_re.append(own(parity, from_left, from_right))
                beyond_im.append(shifts.pair_swap(own(parity, from_right, from_left)))
            total = staple_term(
                total, load(bonds, (parity, 5), rows_later), load(bonds, (parity, 5), rows),
                (beyond_re, beyond_im))
            links = load(field, (parity,), rows)
            product = times(links, total)
            for plane, (upper, lower) in enumerate(PLANES):
                base = pl.multiple_of(16 * block, 16)
                turn = [
                    own(parity, turn_raw[sweep, plane, k, pl.ds(base, 8, stride=2), :],
                        turn_raw[sweep, plane, k, pl.ds(base + 1, 8, stride=2), :])
                    for k in range(4)]
                quat = reflected(product, upper, lower, turn)
                links = rotate_rows(links, upper, lower, quat)
                if plane < 2:
                    product = rotate_rows(product, upper, lower, quat)
            for k in range(9):
                field[parity, k, rows, :] = links[0][k]
                field[parity, 9 + k, rows, :] = links[1][k]

            @pl.when(number < halves - 1)
            def _():
                pack(number + 1, block, parity, links)
                for side, target in ((0, left), (1, right)):
                    send_halo(number + 1, block, side, target)

    def send_loops(sweep, parity):
        low = shifts.low_rows
        number = 2 * sweep + parity
        even, uneven = [], []
        for entry in range(18):
            a = field[parity, entry, pl.ds(0, 8), :]
            b = field[parity, entry, pl.ds(4, 8), :]
            c = field[parity, entry, pl.ds(8, 8), :]
            even.append(jnp.where(low, a, b))
            uneven.append(jnp.where(low, b, c))
        re, im = times(split(even), split(uneven))
        re, im = times((re, im), ([turn_rows(v, 4) for v in re], [turn_rows(v, 4) for v in im]))
        for entry, value in enumerate(re + im):
            loop_rows[pl.ds(8 * entry, 8), :] = value
        for j in range(3):
            for third in range(3):
                loop_out[number, j, pl.ds(8 * third, 8), :] = (
                    loop_rows[pl.ds(64 * third + j, 8, stride=8), :])

        def loop_to(peer_x):
            at = pl.multiple_of(24 * (2 * ix + parity), 8)
            return (
                loop_out.at[number, peer_x - 1, pl.ds(0, 18), :],
                loop_in.at[sweep, iz, pl.ds(at, 18), :])

        for step in range(nx * nz):
            if step == 0:
                @pl.when(ix > 0)
                def _():
                    pltpu.make_async_copy(*loop_to(ix), local_sem.at[number]).start()
            else:
                peer = lax.rem(slab + step, nx * nz)
                peer_x, peer_z = peer // nz, lax.rem(peer, nz)

                @pl.when(peer_x > 0)
                def _():
                    remote(
                        *loop_to(peer_x), loop_sent.at[number], loop_got.at[number],
                        (peer_x, peer_z, ia)).start()

    @pl.loop(0, SWEEPS)
    def _(sweep):
        for parity in (0, 1):
            half_sweep(sweep, parity)
            send_loops(sweep, parity)

    def normalized(load, store, log):
        square = None
        for k in range(162):
            value = load(k)
            square = value * value if square is None else square + value * value
        rms = jnp.sqrt(square / 162.0 + 1e-06)
        inv = 1.0 / rms
        for k in range(162):
            store(k, load(k) * inv)
        return log + jnp.log(rms)

    def combine(left_ref, right_ref, dst_ref, keep):
        for k in range(81):
            sums[k] = right_ref[k] + right_ref[81 + k]

        @pl.loop(0, 9)
        def _(row):
            for third in range(3):
                columns = range(3 * third, 3 * third + 3)
                acc = [[None] * 3 for _ in columns]
                for mid in range(9):
                    a_re, a_im = left_ref[9 * row + mid], left_ref[81 + 9 * row + mid]
                    a_sum = a_re + a_im
                    for place, col in enumerate(columns):
                        at = 9 * mid + col
                        terms = (a_re * right_ref[at], a_im * right_ref[81 + at], a_sum * sums[at])
                        for slot, term in enumerate(terms):
                            old = acc[place][slot]
                            acc[place][slot] = term if old is None else old + term
                for place, col in enumerate(columns):
                    plain, cross, both = acc[place]
                    dst_ref[9 * row + col] = plain - cross
                    dst_ref[81 + 9 * row + col] = both - plain - cross
        log = normalized(
            lambda k: dst_ref[k], lambda k, value: dst_ref.__setitem__(k, keep(k, value)),
            left_ref[162] + right_ref[162])
        dst_ref[162] = keep(162, log)

    def result_to(target):
        lanes = pl.ds(pl.multiple_of(LANES * (ix - 1), LANES), LANES)
        rows = pl.ds(2 * target, 2)
        return (
            (final.at[pl.ds(0, 162), rows, :], out_hbm.at[:, :, lanes]),
            (final.at[162, rows, :], log_hbm.at[:, lanes]))

    @pl.when(ix > 0)
    def _():
        def await_loops(number):
            ref = loop_out.at[number, 0, pl.ds(0, 18), :]
            landed(ref, local_sem.at[number])
            landed(space_raw.at[0, :, pl.ds(0, 15), :], loop_got.at[number])

        def add_operator(slot, sweep):
            to = jnp.where(slot == 0, 0, slot + 3)
            loops = [loop_in[sweep, slot, pl.ds(k, 8, stride=24), :] for k in range(18)]
            partner = [shifts.deep(value, 4) for value in loops]
            for a in range(3):
                for c in range(3):
                    for e in range(3):
                        for d in range(3):
                            l_re, l_im = loops[3 * a + e], loops[9 + 3 * a + e]
                            r_re, r_im = partner[3 * c + d], partner[9 + 3 * c + d]
                            re = l_re * r_re + l_im * r_im
                            im = l_im * r_re - l_re * r_im
                            at = 9 * (3 * a + c) + 3 * e + d
                            if sweep:
                                re = oper[to, at] + re
                                im = oper[to, 81 + at] + im
                            oper[to, at] = re
                            oper[to, 81 + at] = im
            return to

        for sweep in range(SWEEPS):
            await_loops(2 * sweep)
            await_loops(2 * sweep + 1)

            @pl.loop(0, nz)
            def _(slot):
                to = add_operator(slot, sweep)
                if sweep == SWEEPS - 1:
                    third = 1.0 / SWEEPS
                    log = normalized(
                        lambda k: oper[to, k] * third,
                        lambda k, value: oper.at[to].__setitem__(k, value),
                        jnp.zeros((8, LANES)))
                    oper[to, 162] = log

        @pl.loop(1, nz)
        def _(slot):
            combine(oper.at[slot - 1], oper.at[slot + 3], oper.at[slot], lambda k, value: value)

        row = lax.broadcasted_iota(jnp.int32, (8, LANES), 0)

        def moved(value, k, rows):
            unit = 1.0 if k < 81 and k % 10 == 0 else 0.0
            return jnp.where(row < rows, unit, turn_rows(value, -rows))

        def by_column(k, value):
            swapped = jnp.where(row % 2 == 0, turn_rows(value, 1), turn_rows(value, -1))
            return jnp.where(odd, swapped, value)

        for k in range(163):
            chain_a[k] = moved(oper[nz - 1, k], k, 2)
            chain_b[k] = moved(chain_a[k], k, 2)
        combine(chain_b, chain_a, group, lambda k, value: jnp.where(row < 2, chain_a[k], value))
        for k in range(163):
            chain_b[k] = moved(group[k], k, 4)
        combine(chain_b, group, chain_a, lambda k, value: jnp.where(row < 4, group[k], value))
        combine(chain_a, oper.at[iz], final, by_column)

        for target in range(nx):
            @pl.when(ix == target)
            def _():
                for piece, (src, dst) in enumerate(result_to(target)):
                    pltpu.make_async_copy(src, dst, done_sem.at[piece]).start()

            @pl.when(ix != target)
            def _():
                for piece, (src, dst) in enumerate(result_to(target)):
                    remote(
                        src, dst, done_sem.at[2 + piece], back_sem.at[piece, ix], (target, iz, ia)
                    ).start()
        for piece, (src, dst) in enumerate(result_to(0)):
            pltpu.make_async_copy(src, dst, done_sem.at[piece]).wait()

    for source in range(1, nx):
        @pl.when(ix != source)
        def _():
            landed(final.at[pl.ds(0, 162), pl.ds(0, 2), :], back_sem.at[0, source])
            landed(final.at[162, pl.ds(0, 2), :], back_sem.at[1, source])

    for piece, cover in enumerate(covers):
        landed(cover, edge_out.at[piece])
    for number in range(halves):
        for block in range(2):
            for side in range(2):
                await_halo(halo_out, number, block, side)

    @pl.when(ix == 0)
    def _():
        for number in range(halves):
            landed(space_raw.at[0, :, pl.ds(0, 12), :], loop_sent.at[number])

    @pl.when(ix > 0)
    def _():
        for number in range(halves):
            landed(space_raw.at[0, :, pl.ds(0, 11), :], loop_sent.at[number])
        landed(final.at[pl.ds(0, 162), pl.ds(0, 6), :], done_sem.at[2])
        landed(final.at[162, pl.ds(0, 6), :], done_sem.at[3])


def finish(transfer_in, log_in, transfer_out, log_out, held, log_held, sem_in, sem_out):
    pieces = [
        (transfer_in.at[pl.ds(27 * k, 27)], held.at[pl.ds(27 * k, 27)],
         transfer_out.at[pl.ds(27 * k, 27)])
        for k in range(6)
    ] + [(log_in, log_held, log_out)]
    ins = [pltpu.make_async_copy(src, mid, sem_in.at[k]) for k, (src, mid, _) in enumerate(pieces)]
    outs = [
        pltpu.make_async_copy(mid, dst, sem_out.at[k]) for k, (_, mid, dst) in enumerate(pieces)]
    for copy in ins:
        copy.start()
    for arrived, leaving in zip(ins, outs):
        arrived.wait()
        leaving.start()
    for copy in outs:
        copy.wait()


def per_device(temporal_links, spatial_links, rotations):
    f32, dma = jnp.float32, pltpu.SemaphoreType.DMA
    halves = 2 * SWEEPS
    transfer, log_scale = pl.pallas_call(
        kernel,
        name="slab_chain",
        out_shape=(
            jax.ShapeDtypeStruct((162, 2, 3 * LANES), f32),
            jax.ShapeDtypeStruct((2, 3 * LANES), f32),
        ),
        in_specs=[pl.BlockSpec(memory_space=pl.ANY)] * 3,
        out_specs=[pl.BlockSpec(memory_space=pl.ANY)] * 2,
        scratch_shapes=[
            pltpu.VMEM((18, 32, LANES), f32),
            pltpu.VMEM((3, 18, 48, LANES), f32),
            pltpu.VMEM((3, 3, 4, 32, LANES), f32),
            pltpu.VMEM((12, 16, LANES), f32),
            pltpu.VMEM((12, 16, LANES), f32),
            pltpu.VMEM((12, 8, LANES), f32),
            pltpu.VMEM((2, 18, 16, LANES), f32),
            pltpu.VMEM((2, 6, 18, 24, LANES), f32),
            pltpu.VMEM((4, 18, 8, LANES), f32),
            pltpu.VMEM((halves, 2, 2, 9, 8, LANES), f32),
            pltpu.VMEM((halves, 2, 2, 9, 8, LANES), f32),
            pltpu.VMEM((192, LANES), f32),
            pltpu.VMEM((halves, 3, 24, LANES), f32),
            pltpu.VMEM((SWEEPS, 4, 192, LANES), f32),
            pltpu.VMEM((7, 163, 8, LANES), f32),
            pltpu.VMEM((163, 8, LANES), f32),
            pltpu.VMEM((163, 8, LANES), f32),
            pltpu.VMEM((163, 8, LANES), f32),
            pltpu.VMEM((81, 8, LANES), f32),
            pltpu.VMEM((163, 8, LANES), f32),
            dma((3,)), dma((4,)), dma((4,)), dma((halves, 2, 2)), dma((halves, 2, 2)),
            dma((halves,)), dma((halves,)), dma((halves,)), dma((2, 4)), dma((4,)),
        ],
        compiler_params=pltpu.CompilerParams(collective_id=0, has_side_effects=True),
    )(temporal_links, spatial_links, rotations)
    transfer, log_scale = pl.pallas_call(
        finish,
        name="hand_over",
        out_shape=(
            jax.ShapeDtypeStruct((162, 2, 3 * LANES), f32),
            jax.ShapeDtypeStruct((2, 3 * LANES), f32),
        ),
        in_specs=[pl.BlockSpec(memory_space=pl.ANY)] * 2,
        out_specs=[pl.BlockSpec(memory_space=pl.ANY)] * 2,
        scratch_shapes=[
            pltpu.VMEM((162, 2, 3 * LANES), f32), pltpu.VMEM((2, 3 * LANES), f32),
            dma((7,)), dma((7,)),
        ],
    )(transfer, log_scale)
    return transfer.reshape(2, 9, 9, 1, 2, 3 * LANES), log_scale.reshape(1, 2, 3 * LANES)


def solution(mesh):
    split = Mesh(mesh.devices.reshape(4, 4, mesh.shape["sa"]), AXES)
    slabs = ("ta_0", "ta_1")
    return jax.shard_map(
        per_device,
        mesh=split,
        in_specs=(
            P(None, slabs, "sa", None),
            P(None, None, slabs, "sa", None),
            P(None, None, None, slabs, "sa", None),
        ),
        out_specs=(P(None, None, None, slabs, "sa", None), P(slabs, "sa", None)),
        check_vma=False,
    )
```

```python
import jax
import jax.numpy as jnp
from jax import lax
from jax.experimental import pallas as pl
from jax.experimental.pallas import tpu as pltpu
from jax.sharding import Mesh
from jax.sharding import PartitionSpec as P

SWEEPS = 3
LZ = 16
LANES = 128
MESH = pl.DeviceIdType.MESH
AXES = ("ta_0", "ta_1", "sa")
PLANES = ((0, 1), (1, 2), (0, 2))


def times(left, right):
    out_re, out_im = [], []
    for row in range(3):
        for col in range(3):
            re = im = None
            for mid in range(3):
                a_re, a_im = left[0][3 * row + mid], left[1][3 * row + mid]
                b_re, b_im = right[0][3 * mid + col], right[1][3 * mid + col]
                p_re = a_re * b_re - a_im * b_im
                p_im = a_re * b_im + a_im * b_re
                re = p_re if re is None else re + p_re
                im = p_im if im is None else im + p_im
            out_re.append(re)
            out_im.append(im)
    return out_re, out_im


def staple_term(total, later, now, link):
    total_re, total_im = list(total[0]), list(total[1])
    for col in range(3):
        mid_re, mid_im = [], []
        for k in range(3):
            re = im = None
            for m in range(3):
                a_re, a_im = now[0][3 * col + m], now[1][3 * col + m]
                b_re, b_im = link[0][3 * m + k], link[1][3 * m + k]
                p_re = a_re * b_re - a_im * b_im
                p_im = a_re * b_im + a_im * b_re
                re = p_re if re is None else re + p_re
                im = p_im if im is None else im + p_im
            mid_re.append(re)
            mid_im.append(im)
        for row in range(3):
            re, im = total_re[3 * row + col], total_im[3 * row + col]
            for k in range(3):
                a_re, a_im = later[0][3 * row + k], later[1][3 * row + k]
                p_re = a_re * mid_re[k] + a_im * mid_im[k]
                p_im = a_im * mid_re[k] - a_re * mid_im[k]
                re = p_re if re is None else re + p_re
                im = p_im if im is None else im + p_im
            total_re[3 * row + col], total_im[3 * row + col] = re, im
    return total_re, total_im


def dagger(matrix):
    order = (0, 3, 6, 1, 4, 7, 2, 5, 8)
    return [matrix[0][k] for k in order], [-matrix[1][k] for k in order]


def rotate_rows(matrix, upper, lower, quat):
    q0, q1, q2, q3 = quat
    re, im = list(matrix[0]), list(matrix[1])
    for col in range(3):
        u_re, u_im = matrix[0][3 * upper + col], matrix[1][3 * upper + col]
        l_re, l_im = matrix[0][3 * lower + col], matrix[1][3 * lower + col]
        re[3 * upper + col] = q0 * u_re - q3 * u_im + q2 * l_re - q1 * l_im
        im[3 * upper + col] = q0 * u_im + q3 * u_re + q2 * l_im + q1 * l_re
        re[3 * lower + col] = q0 * l_re + q3 * l_im - q2 * u_re - q1 * u_im
        im[3 * lower + col] = q0 * l_im - q3 * l_re - q2 * u_im + q1 * u_re
    return re, im


def reflected(product, upper, lower, turn):
    re, im = product
    uu, ul, lu, ll = 4 * upper, 3 * upper + lower, 3 * lower + upper, 4 * lower
    w0 = 0.5 * (re[uu] + re[ll])
    w1 = 0.5 * (im[ul] + im[lu])
    w2 = 0.5 * (re[ul] - re[lu])
    w3 = 0.5 * (im[uu] - im[ll])
    vec_sq = w1 * w1 + w2 * w2 + w3 * w3
    w0_sq = w0 * w0
    inv = 1.0 / jnp.maximum(w0_sq + vec_sq, 0.5)
    scale = -2.0 * w0 * inv
    r0, r1, r2, r3 = (w0_sq - vec_sq) * inv, scale * w1, scale * w2, scale * w3
    x0, x1, x2, x3 = turn
    return (
        x0 * r0 - (x1 * r1 + x2 * r2 + x3 * r3),
        x0 * r1 + r0 * x1 - (x2 * r3 - x3 * r2),
        x0 * r2 + r0 * x2 - (x3 * r1 - x1 * r3),
        x0 * r3 + r0 * x3 - (x1 * r2 - x2 * r1),
    )


def closed(six):
    re, im = list(six[0]), list(six[1])
    for col in range(3):
        a, b = (col + 1) % 3, (col + 2) % 3
        real = (re[a] * re[3 + b] - im[a] * im[3 + b]) - (re[b] * re[3 + a] - im[b] * im[3 + a])
        imag = (re[a] * im[3 + b] + im[a] * re[3 + b]) - (re[b] * im[3 + a] + im[b] * re[3 + a])
        re.append(real)
        im.append(-imag)
    return re, im


def turn_lanes(value, steps):
    return pltpu.roll(value, (-steps) % LANES, 1)


def turn_rows(value, steps):
    return pltpu.roll(value, (-steps) % 8, 0)


class Shifts:
    def __init__(self):
        lane = lax.broadcasted_iota(jnp.int32, (8, LANES), 1)
        row = lax.broadcasted_iota(jnp.int32, (8, LANES), 0)
        self.depth = lane % LZ
        self.lane = lane
        self.slot = row % 4
        self.odd = ((lane // LZ + lane) % 2) == 1
        self.low_rows = row < 4
        self.even_lane = lane % 2 == 0

    def rows(self, value, offset):
        if offset > 0:
            turned = turn_lanes(value, LZ)
            after = jnp.where(self.slot == 2, turn_rows(turned, -2), turn_rows(turned, 1))
            return jnp.where(self.lane < LANES - LZ, turned, after)
        turned = turn_lanes(value, -LZ)
        before = jnp.where(self.slot == 0, turn_rows(turned, 2), turn_rows(turned, -1))
        return jnp.where(self.lane >= LZ, turned, before)

    def deep(self, value, offset):
        if offset > 0:
            return jnp.where(
                self.depth < LZ - offset, turn_lanes(value, offset), turn_lanes(value, offset - LZ)
            )
        return jnp.where(
            self.depth >= -offset, turn_lanes(value, offset), turn_lanes(value, LZ + offset)
        )

    def pair_swap(self, value):
        return jnp.where(self.even_lane, turn_lanes(value, 1), turn_lanes(value, -1))


def kernel(
    time_hbm, space_hbm, turn_hbm, out_hbm, log_hbm,
    time_raw, space_raw, turn_raw, left_out, left_in, left_next,
    field, bonds, shifted, pack_out, pack_in, loop_rows, loop_out, loop_in,
    oper, chain_a, chain_b, group, sums, final,
    in_sem, edge_out, edge_in, halo_out, halo_in, loop_sent, loop_got, local_sem, back_sem, done_sem,
    known,
):
    ix, iz, ia = lax.axis_index("ta_0"), lax.axis_index("ta_1"), lax.axis_index("sa")
    nx, nz, na = 4, 4, lax.axis_size("sa")
    left, right = lax.rem(ia + na - 1, na), lax.rem(ia + 1, na)
    slab = ix * nz + iz
    earlier = lax.rem(slab + nx * nz - 1, nx * nz)
    later = lax.rem(slab + 1, nx * nz)
    earlier_x, earlier_z = earlier // nz, lax.rem(earlier, nz)
    later_x, later_z = later // nz, lax.rem(later, nz)
    halves = 2 * SWEEPS

    for t in range(4):
        for j in range(3):
            lanes, rows = pl.ds(LANES * j, LANES), pl.ds(8 * t + 2 * j, 2)
            pltpu.make_async_copy(
                time_hbm.at[:, t, :, lanes], time_raw.at[:, rows, :], in_sem.at[0]).start()
            pltpu.make_async_copy(
                space_hbm.at[:, :, t, :, lanes], space_raw.at[:, :, rows, :], in_sem.at[1]).start()
    for t in range(4):
        for j in range(3):
            lanes, rows = pl.ds(LANES * j, LANES), pl.ds(8 * t + 2 * j, 2)
            pltpu.make_async_copy(
                turn_hbm.at[:, :, :, t, :, lanes], turn_raw.at[:, :, :, rows, :], in_sem.at[2]
            ).start()

    barrier = pltpu.get_barrier_semaphore()
    peers = [(ix, iz, left), (ix, iz, right)]
    peers += [(earlier_x, earlier_z, ia), (later_x, later_z, ia)]
    peers += [(earlier_x, earlier_z, right), (later_x, later_z, left)]
    for peer in peers:
        pl.semaphore_signal(barrier, inc=1, device_id=peer, device_id_type=MESH)

    def remote(src, dst, out_sem, got_sem, target):
        return pltpu.make_async_remote_copy(
            src_ref=src, dst_ref=dst, send_sem=out_sem, recv_sem=got_sem,
            device_id=target, device_id_type=MESH)

    def landed(ref, sem):
        pltpu.make_async_copy(ref, ref, sem).wait()

    def tell(stage):
        for side, step in ((0, 1 << stage), (1, nx * nz - (1 << stage))):
            peer = lax.rem(slab + step, nx * nz)
            pl.semaphore_signal(
                known.at[stage, side], inc=1, device_id=(peer // nz, lax.rem(peer, nz), ia),
                device_id_type=MESH)

    def hear(stage):
        for side in range(2):
            pl.semaphore_wait(known.at[stage, side], 1)

    shifts = Shifts()
    odd = shifts.odd

    def own(parity, first, second):
        return jnp.where(odd, first, second) if parity else jnp.where(odd, second, first)

    def split(values):
        return values[:9], values[9:]

    def pack(number, block, parity, links):
        for k in range(9):
            real, partner = links[0][k], shifts.pair_swap(links[1][k])
            pack_out[number, block, 0, k] = own(parity, real, partner)
            pack_out[number, block, 1, k] = own(parity, partner, real)

    def send_halo(number, block, side, target):
        for at in (0, 4):
            rows = pl.ds(at, 3)
            remote(
                pack_out.at[number, block, side, :, rows, :],
                pack_in.at[number, block, side, :, rows, :],
                halo_out.at[number, block, side], halo_in.at[number, block, side],
                (ix, iz, target)).start()

    def await_halo(sem, number, block, side):
        landed(pack_in.at[number, block, side, :, pl.ds(0, 6), :], sem.at[number, block, side])

    two_rows = [*range(6), *range(9, 15)]
    landed(space_raw.at[:, :, pl.ds(0, 24), :], in_sem.at[1])
    for block in range(2):
        for place, entry in enumerate(two_rows):
            left_out[place, pl.ds(8 * block, 8), :] = (
                space_raw[0, entry, pl.ds(16 * block + 1, 8, stride=2), :])
    landed(time_raw.at[:, pl.ds(0, 24), :], in_sem.at[0])
    for block in range(2):
        packed = []
        for entry in range(18):
            first = time_raw[entry, pl.ds(16 * block, 8, stride=2), :]
            second = time_raw[entry, pl.ds(16 * block + 1, 8, stride=2), :]
            field[0, entry, pl.ds(8 * block, 8), :] = own(0, first, second)
            value = own(1, first, second)
            field[1, entry, pl.ds(8 * block, 8), :] = value
            packed.append(value)
        pack(0, block, 1, split(packed))
    pl.semaphore_wait(barrier, len(peers))
    for block in range(2):
        for side, target in ((0, left), (1, right)):
            send_halo(0, block, side, target)
    edges = []
    for t in range(4):
        rows = pl.ds(4 * t, 3)
        edges.append(remote(
            left_out.at[:, rows, :], left_in.at[:, rows, :], edge_out.at[0], edge_in.at[0],
            (ix, iz, right)))
    for half in range(2):
        rows = pl.ds(0, 6)
        edges.append(remote(
            space_raw.at[:, pl.ds(9 * half, 6), rows, :],
            space_raw.at[:, pl.ds(9 * half, 6), pl.ds(32, 6), :],
            edge_out.at[1 + half], edge_in.at[1 + half], (earlier_x, earlier_z, ia)))
    edges.append(remote(
        left_out.at[:, pl.ds(0, 3), :], left_next.at[:, pl.ds(0, 3), :],
        edge_out.at[3], edge_in.at[3], (earlier_x, earlier_z, right)))
    for copy in edges:
        copy.start()
    tell(0)
    covers = (
        left_in.at[:, pl.ds(0, 12), :], space_raw.at[:, pl.ds(0, 6), pl.ds(0, 6), :],
        space_raw.at[:, pl.ds(0, 6), pl.ds(0, 6), :], left_in.at[:, pl.ds(0, 3), :])

    def raw(direction, at, column):
        return [space_raw[direction, k, pl.ds(at + column, 8, stride=2), :] for k in range(18)]

    def inner_bonds(block):
        at, to = 16 * block, pl.ds(8 * block, 8)
        if not isinstance(block, int):
            at, to = pl.multiple_of(at, 16), pl.ds(pl.multiple_of(8 * block, 8), 8)

        def put(parity, place, matrix):
            for k in range(9):
                bonds[parity, place, k, to, :] = matrix[0][k]
                bonds[parity, place, 9 + k, to, :] = matrix[1][k]

        inner = raw(0, at, 0)
        inner_dag = dagger(split(inner))
        inner_dag = inner_dag[0] + inner_dag[1]
        for parity in (0, 1):
            put(parity, 0, split([own(parity, a, b) for a, b in zip(inner, inner_dag)]))
        for direction, shift in ((1, shifts.rows), (2, shifts.deep)):
            first, second = raw(direction, at, 0), raw(direction, at, 1)
            for parity in (0, 1):
                here = [own(parity, a, b) for a, b in zip(first, second)]
                put(parity, 2 * direction - 1, split(here))
                back = [shift(value, -1) for value in here]
                put(1 - parity, 2 * direction, dagger(split(back)))

    def outer_bonds(block):
        to = pl.ds(8 * block, 8)
        outer = raw(0, 16 * block, 1)
        if block < 2:
            six = [left_in[k, to, :] for k in range(12)]
        else:
            six = [left_next[k] for k in range(12)]
        beyond = dagger(closed((six[:6], six[6:])))
        beyond = beyond[0] + beyond[1]
        for parity in (0, 1):
            for k in range(18):
                bonds[parity, 5, k, to, :] = own(parity, beyond[k], outer[k])

    @pl.loop(0, 2)
    def _(block):
        inner_bonds(block)

    landed(turn_raw.at[:, :, :, pl.ds(0, 24), :], in_sem.at[2])
    landed(covers[0], edge_in.at[0])
    for block in range(2):
        outer_bonds(block)
    hear(0)
    tell(1)

    def half_sweep(sweep, parity):
        number = 2 * sweep + parity

        @pl.loop(0, 2)
        def _(block):
            rows = pl.ds(pl.multiple_of(8 * block, 8), 8)
            rows_later = pl.ds(8 * block + 4, 8)

            if parity == 0:
                @pl.when(jnp.logical_and(sweep == 0, block == 1))
                def _():
                    for piece in range(1, 4):
                        landed(covers[piece], edge_in.at[piece])
                    hear(1)
                    tell(2)
                    for direction in range(3):
                        six = [space_raw[direction, k, pl.ds(32, 8), :] for k in two_rows]
                        re, im = closed((six[:6], six[6:]))
                        for k in range(6, 9):
                            space_raw[direction, k, pl.ds(32, 8), :] = re[k]
                            space_raw[direction, 9 + k, pl.ds(32, 8), :] = im[k]
                    inner_bonds(2)
                    outer_bonds(2)

            def load(ref, lead, where):
                return split([ref[(*lead, k, where, slice(None))] for k in range(18)])

            for entry in range(18):
                value = field[1 - parity, entry, rows, :]
                shifted[0, entry] = shifts.rows(value, 1)
                shifted[1, entry] = shifts.rows(value, -1)
                shifted[2, entry] = shifts.deep(value, 1)
                shifted[3, entry] = shifts.deep(value, -1)
            total = ([None] * 9, [None] * 9)
            total = staple_term(
                total, load(bonds, (parity, 0), rows_later), load(bonds, (parity, 0), rows),
                load(field, (1 - parity,), rows))
            for place in range(1, 5):
                total = staple_term(
                    total, load(bonds, (parity, place), rows_later),
                    load(bonds, (parity, place), rows),
                    load(shifted, (place - 1,), slice(None)))

            for side in range(2):
                await_halo(halo_in, number, block, side)
            beyond_re, beyond_im = [], []
            for k in range(9):
                from_left = pack_in[number, block, 1, k]
                from_right = pack_in[number, block, 0, k]
                beyond_re.append(own(parity, from_left, from_right))
                beyond_im.append(shifts.pair_swap(own(parity, from_right, from_left)))
            total = staple_term(
                total, load(bonds, (parity, 5), rows_later), load(bonds, (parity, 5), rows),
                (beyond_re, beyond_im))
            links = load(field, (parity,), rows)
            product = times(links, total)
            for plane, (upper, lower) in enumerate(PLANES):
                base = pl.multiple_of(16 * block, 16)
                turn = [
                    own(parity, turn_raw[sweep, plane, k, pl.ds(base, 8, stride=2), :],
                        turn_raw[sweep, plane, k, pl.ds(base + 1, 8, stride=2), :])
                    for k in range(4)]
                quat = reflected(product, upper, lower, turn)
                links = rotate_rows(links, upper, lower, quat)
                if plane < 2:
                    product = rotate_rows(product, upper, lower, quat)
            for k in range(9):
                field[parity, k, rows, :] = links[0][k]
                field[parity, 9 + k, rows, :] = links[1][k]

            @pl.when(number < halves - 1)
            def _():
                pack(number + 1, block, parity, links)
                for side, target in ((0, left), (1, right)):
                    send_halo(number + 1, block, side, target)

    def send_loops(sweep, parity):
        low = shifts.low_rows
        number = 2 * sweep + parity
        even, uneven = [], []
        for entry in range(18):
            a = field[parity, entry, pl.ds(0, 8), :]
            b = field[parity, entry, pl.ds(4, 8), :]
            c = field[parity, entry, pl.ds(8, 8), :]
            even.append(jnp.where(low, a, b))
            uneven.append(jnp.where(low, b, c))
        re, im = times(split(even), split(uneven))
        re, im = times((re, im), ([turn_rows(v, 4) for v in re], [turn_rows(v, 4) for v in im]))
        for entry, value in enumerate(re + im):
            loop_rows[pl.ds(8 * entry, 8), :] = value
        for j in range(3):
            for third in range(3):
                loop_out[number, j, pl.ds(8 * third, 8), :] = (
                    loop_rows[pl.ds(64 * third + j, 8, stride=8), :])

        def loop_to(peer_x):
            at = pl.multiple_of(24 * (2 * ix + parity), 8)
            return (
                loop_out.at[number, peer_x - 1, pl.ds(0, 18), :],
                loop_in.at[sweep, iz, pl.ds(at, 18), :])

        for step_z, step_x in [(z, x) for z in (2, 1, 3, 0) for x in (2, 1, 3, 0)]:
            if step_z == step_x == 0:
                @pl.when(ix > 0)
                def _():
                    pltpu.make_async_copy(*loop_to(ix), local_sem.at[number]).start()
            else:
                peer_x, peer_z = lax.rem(ix + step_x, nx), lax.rem(iz + step_z, nz)

                @pl.when(peer_x > 0)
                def _():
                    remote(
                        *loop_to(peer_x), loop_sent.at[number], loop_got.at[number],
                        (peer_x, peer_z, ia)).start()

    @pl.loop(0, SWEEPS)
    def _(sweep):
        for parity in (0, 1):
            half_sweep(sweep, parity)
            if parity == 0:
                @pl.when(sweep == 0)
                def _():
                    hear(2)
            send_loops(sweep, parity)

    def normalized(load, store, log):
        square = None
        for k in range(162):
            value = load(k)
            square = value * value if square is None else square + value * value
        rms = jnp.sqrt(square / 162.0 + 1e-06)
        inv = 1.0 / rms
        for k in range(162):
            store(k, load(k) * inv)
        return log + jnp.log(rms)

    def combine(left_ref, right_ref, dst_ref, keep):
        for k in range(81):
            sums[k] = right_ref[k] + right_ref[81 + k]

        @pl.loop(0, 9)
        def _(row):
            for third in range(3):
                columns = range(3 * third, 3 * third + 3)
                acc = [[None] * 3 for _ in columns]
                for mid in range(9):
                    a_re, a_im = left_ref[9 * row + mid], left_ref[81 + 9 * row + mid]
                    a_sum = a_re + a_im
                    for place, col in enumerate(columns):
                        at = 9 * mid + col
                        terms = (a_re * right_ref[at], a_im * right_ref[81 + at], a_sum * sums[at])
                        for slot, term in enumerate(terms):
                            old = acc[place][slot]
                            acc[place][slot] = term if old is None else old + term
                for place, col in enumerate(columns):
                    plain, cross, both = acc[place]
                    dst_ref[9 * row + col] = plain - cross
                    dst_ref[81 + 9 * row + col] = both - plain - cross
        log = normalized(
            lambda k: dst_ref[k], lambda k, value: dst_ref.__setitem__(k, keep(k, value)),
            left_ref[162] + right_ref[162])
        dst_ref[162] = keep(162, log)

    def result_to(target):
        lanes = pl.ds(pl.multiple_of(LANES * (ix - 1), LANES), LANES)
        rows = pl.ds(2 * target, 2)
        return (
            (final.at[pl.ds(0, 162), rows, :], out_hbm.at[:, :, lanes]),
            (final.at[162, rows, :], log_hbm.at[:, lanes]))

    @pl.when(ix > 0)
    def _():
        def await_loops(number):
            ref = loop_out.at[number, 0, pl.ds(0, 18), :]
            landed(ref, local_sem.at[number])
            landed(space_raw.at[0, :, pl.ds(0, 15), :], loop_got.at[number])

        def add_operator(slot, sweep):
            to = jnp.where(slot == 0, 0, slot + 3)
            loops = [loop_in[sweep, slot, pl.ds(k, 8, stride=24), :] for k in range(18)]
            partner = [shifts.deep(value, 4) for value in loops]
            for a in range(3):
                for c in range(3):
                    for e in range(3):
                        for d in range(3):
                            l_re, l_im = loops[3 * a + e], loops[9 + 3 * a + e]
                            r_re, r_im = partner[3 * c + d], partner[9 + 3 * c + d]
                            re = l_re * r_re + l_im * r_im
                            im = l_im * r_re - l_re * r_im
                            at = 9 * (3 * a + c) + 3 * e + d
                            if sweep:
                                re = oper[to, at] + re
                                im = oper[to, 81 + at] + im
                            oper[to, at] = re
                            oper[to, 81 + at] = im
            return to

        for sweep in range(SWEEPS):
            await_loops(2 * sweep)
            await_loops(2 * sweep + 1)

            @pl.loop(0, nz)
            def _(slot):
                to = add_operator(slot, sweep)
                if sweep == SWEEPS - 1:
                    third = 1.0 / SWEEPS
                    log = normalized(
                        lambda k: oper[to, k] * third,
                        lambda k, value: oper.at[to].__setitem__(k, value),
                        jnp.zeros((8, LANES)))
                    oper[to, 162] = log

        @pl.loop(1, nz)
        def _(slot):
            combine(oper.at[slot - 1], oper.at[slot + 3], oper.at[slot], lambda k, value: value)

        row = lax.broadcasted_iota(jnp.int32, (8, LANES), 0)

        def moved(value, k, rows):
            unit = 1.0 if k < 81 and k % 10 == 0 else 0.0
            return jnp.where(row < rows, unit, turn_rows(value, -rows))

        def by_column(k, value):
            swapped = jnp.where(row % 2 == 0, turn_rows(value, 1), turn_rows(value, -1))
            return jnp.where(odd, swapped, value)

        for k in range(163):
            chain_a[k] = moved(oper[nz - 1, k], k, 2)
            chain_b[k] = moved(chain_a[k], k, 2)
        combine(chain_b, chain_a, group, lambda k, value: jnp.where(row < 2, chain_a[k], value))
        for k in range(163):
            chain_b[k] = moved(group[k], k, 4)
        combine(chain_b, group, chain_a, lambda k, value: jnp.where(row < 4, group[k], value))
        combine(chain_a, oper.at[iz], final, by_column)

        for target in range(nx):
            @pl.when(ix == target)
            def _():
                for piece, (src, dst) in enumerate(result_to(target)):
                    pltpu.make_async_copy(src, dst, done_sem.at[piece]).start()

            @pl.when(ix != target)
            def _():
                for piece, (src, dst) in enumerate(result_to(target)):
                    remote(
                        src, dst, done_sem.at[2 + piece], back_sem.at[piece, ix], (target, iz, ia)
                    ).start()
        for piece, (src, dst) in enumerate(result_to(0)):
            pltpu.make_async_copy(src, dst, done_sem.at[piece]).wait()

    for source in range(1, nx):
        @pl.when(ix != source)
        def _():
            landed(final.at[pl.ds(0, 162), pl.ds(0, 2), :], back_sem.at[0, source])
            landed(final.at[162, pl.ds(0, 2), :], back_sem.at[1, source])

    for piece, cover in enumerate(covers):
        landed(cover, edge_out.at[piece])
    for number in range(halves):
        for block in range(2):
            for side in range(2):
                await_halo(halo_out, number, block, side)

    @pl.when(ix == 0)
    def _():
        for number in range(halves):
            landed(space_raw.at[0, :, pl.ds(0, 12), :], loop_sent.at[number])

    @pl.when(ix > 0)
    def _():
        for number in range(halves):
            landed(space_raw.at[0, :, pl.ds(0, 11), :], loop_sent.at[number])
        landed(final.at[pl.ds(0, 162), pl.ds(0, 6), :], done_sem.at[2])
        landed(final.at[162, pl.ds(0, 6), :], done_sem.at[3])


def per_device(temporal_links, spatial_links, rotations):
    f32, dma = jnp.float32, pltpu.SemaphoreType.DMA
    halves = 2 * SWEEPS
    transfer, log_scale = pl.pallas_call(
        kernel,
        name="slab_chain",
        out_shape=(pltpu.VMEM((162, 2, 3 * LANES), f32), pltpu.VMEM((2, 3 * LANES), f32)),
        in_specs=[pl.BlockSpec(memory_space=pl.ANY)] * 3,
        out_specs=[pl.BlockSpec(memory_space=pltpu.VMEM)] * 2,
        scratch_shapes=[
            pltpu.VMEM((18, 32, LANES), f32),
            pltpu.VMEM((3, 18, 48, LANES), f32),
            pltpu.VMEM((3, 3, 4, 32, LANES), f32),
            pltpu.VMEM((12, 16, LANES), f32),
            pltpu.VMEM((12, 16, LANES), f32),
            pltpu.VMEM((12, 8, LANES), f32),
            pltpu.VMEM((2, 18, 16, LANES), f32),
            pltpu.VMEM((2, 6, 18, 24, LANES), f32),
            pltpu.VMEM((4, 18, 8, LANES), f32),
            pltpu.VMEM((halves, 2, 2, 9, 8, LANES), f32),
            pltpu.VMEM((halves, 2, 2, 9, 8, LANES), f32),
            pltpu.VMEM((192, LANES), f32),
            pltpu.VMEM((halves, 3, 24, LANES), f32),
            pltpu.VMEM((SWEEPS, 4, 192, LANES), f32),
            pltpu.VMEM((7, 163, 8, LANES), f32),
            pltpu.VMEM((163, 8, LANES), f32),
            pltpu.VMEM((163, 8, LANES), f32),
            pltpu.VMEM((163, 8, LANES), f32),
            pltpu.VMEM((81, 8, LANES), f32),
            pltpu.VMEM((163, 8, LANES), f32),
            dma((3,)), dma((4,)), dma((4,)), dma((halves, 2, 2)), dma((halves, 2, 2)),
            dma((halves,)), dma((halves,)), dma((halves,)), dma((2, 4)), dma((4,)),
            pltpu.SemaphoreType.REGULAR((3, 2)),
        ],
        compiler_params=pltpu.CompilerParams(collective_id=0, has_side_effects=True),
    )(temporal_links, spatial_links, rotations)
    return transfer.reshape(2, 9, 9, 1, 2, 3 * LANES), log_scale.reshape(1, 2, 3 * LANES)


def solution(mesh):
    split = Mesh(mesh.devices.reshape(4, 4, mesh.shape["sa"]), AXES)
    slabs = ("ta_0", "ta_1")
    return jax.shard_map(
        per_device,
        mesh=split,
        in_specs=(
            P(None, slabs, "sa", None),
            P(None, None, slabs, "sa", None),
            P(None, None, None, slabs, "sa", None),
        ),
        out_specs=(P(None, None, None, slabs, "sa", None), P(slabs, "sa", None)),
        check_vma=False,
    )
```

```python
import jax
import jax.numpy as jnp
from jax import lax
from jax.experimental import pallas as pl
from jax.experimental.pallas import tpu as pltpu
from jax.sharding import Mesh
from jax.sharding import PartitionSpec as P

SWEEPS = 3
LZ = 16
LANES = 128
MESH = pl.DeviceIdType.MESH
AXES = ("ta_0", "ta_1", "sa")
PLANES = ((0, 1), (1, 2), (0, 2))


def times(left, right):
    out_re, out_im = [], []
    for row in range(3):
        for col in range(3):
            re = im = None
            for mid in range(3):
                a_re, a_im = left[0][3 * row + mid], left[1][3 * row + mid]
                b_re, b_im = right[0][3 * mid + col], right[1][3 * mid + col]
                p_re = a_re * b_re - a_im * b_im
                p_im = a_re * b_im + a_im * b_re
                re = p_re if re is None else re + p_re
                im = p_im if im is None else im + p_im
            out_re.append(re)
            out_im.append(im)
    return out_re, out_im


def staple_term(total, later, now, link):
    total_re, total_im = list(total[0]), list(total[1])
    for col in range(3):
        mid_re, mid_im = [], []
        for k in range(3):
            re = im = None
            for m in range(3):
                a_re, a_im = now[0][3 * col + m], now[1][3 * col + m]
                b_re, b_im = link[0][3 * m + k], link[1][3 * m + k]
                p_re = a_re * b_re - a_im * b_im
                p_im = a_re * b_im + a_im * b_re
                re = p_re if re is None else re + p_re
                im = p_im if im is None else im + p_im
            mid_re.append(re)
            mid_im.append(im)
        for row in range(3):
            re, im = total_re[3 * row + col], total_im[3 * row + col]
            for k in range(3):
                a_re, a_im = later[0][3 * row + k], later[1][3 * row + k]
                p_re = a_re * mid_re[k] + a_im * mid_im[k]
                p_im = a_im * mid_re[k] - a_re * mid_im[k]
                re = p_re if re is None else re + p_re
                im = p_im if im is None else im + p_im
            total_re[3 * row + col], total_im[3 * row + col] = re, im
    return total_re, total_im


def dagger(matrix):
    order = (0, 3, 6, 1, 4, 7, 2, 5, 8)
    return [matrix[0][k] for k in order], [-matrix[1][k] for k in order]


def rotate_rows(matrix, upper, lower, quat):
    q0, q1, q2, q3 = quat
    re, im = list(matrix[0]), list(matrix[1])
    for col in range(3):
        u_re, u_im = matrix[0][3 * upper + col], matrix[1][3 * upper + col]
        l_re, l_im = matrix[0][3 * lower + col], matrix[1][3 * lower + col]
        re[3 * upper + col] = q0 * u_re - q3 * u_im + q2 * l_re - q1 * l_im
        im[3 * upper + col] = q0 * u_im + q3 * u_re + q2 * l_im + q1 * l_re
        re[3 * lower + col] = q0 * l_re + q3 * l_im - q2 * u_re - q1 * u_im
        im[3 * lower + col] = q0 * l_im - q3 * l_re - q2 * u_im + q1 * u_re
    return re, im


def reflected(product, upper, lower, turn):
    re, im = product
    uu, ul, lu, ll = 4 * upper, 3 * upper + lower, 3 * lower + upper, 4 * lower
    w0 = 0.5 * (re[uu] + re[ll])
    w1 = 0.5 * (im[ul] + im[lu])
    w2 = 0.5 * (re[ul] - re[lu])
    w3 = 0.5 * (im[uu] - im[ll])
    vec_sq = w1 * w1 + w2 * w2 + w3 * w3
    w0_sq = w0 * w0
    inv = 1.0 / jnp.maximum(w0_sq + vec_sq, 0.5)
    scale = -2.0 * w0 * inv
    r0, r1, r2, r3 = (w0_sq - vec_sq) * inv, scale * w1, scale * w2, scale * w3
    x0, x1, x2, x3 = turn
    return (
        x0 * r0 - (x1 * r1 + x2 * r2 + x3 * r3),
        x0 * r1 + r0 * x1 - (x2 * r3 - x3 * r2),
        x0 * r2 + r0 * x2 - (x3 * r1 - x1 * r3),
        x0 * r3 + r0 * x3 - (x1 * r2 - x2 * r1),
    )


def closed(six):
    re, im = list(six[0]), list(six[1])
    for col in range(3):
        a, b = (col + 1) % 3, (col + 2) % 3
        real = (re[a] * re[3 + b] - im[a] * im[3 + b]) - (re[b] * re[3 + a] - im[b] * im[3 + a])
        imag = (re[a] * im[3 + b] + im[a] * re[3 + b]) - (re[b] * im[3 + a] + im[b] * re[3 + a])
        re.append(real)
        im.append(-imag)
    return re, im


def turn_lanes(value, steps):
    return pltpu.roll(value, (-steps) % LANES, 1)


def turn_rows(value, steps):
    return pltpu.roll(value, (-steps) % 8, 0)


class Shifts:
    def __init__(self):
        lane = lax.broadcasted_iota(jnp.int32, (8, LANES), 1)
        row = lax.broadcasted_iota(jnp.int32, (8, LANES), 0)
        self.depth = lane % LZ
        self.lane = lane
        self.slot = row % 4
        self.odd = ((lane // LZ + lane) % 2) == 1
        self.low_rows = row < 4
        self.even_lane = lane % 2 == 0

    def rows(self, value, offset):
        if offset > 0:
            turned = turn_lanes(value, LZ)
            after = jnp.where(self.slot == 2, turn_rows(turned, -2), turn_rows(turned, 1))
            return jnp.where(self.lane < LANES - LZ, turned, after)
        turned = turn_lanes(value, -LZ)
        before = jnp.where(self.slot == 0, turn_rows(turned, 2), turn_rows(turned, -1))
        return jnp.where(self.lane >= LZ, turned, before)

    def deep(self, value, offset):
        if offset > 0:
            return jnp.where(
                self.depth < LZ - offset, turn_lanes(value, offset), turn_lanes(value, offset - LZ)
            )
        return jnp.where(
            self.depth >= -offset, turn_lanes(value, offset), turn_lanes(value, LZ + offset)
        )

    def pair_swap(self, value):
        return jnp.where(self.even_lane, turn_lanes(value, 1), turn_lanes(value, -1))


def kernel(
    time_hbm, space_hbm, turn_hbm, out_hbm, log_hbm,
    time_raw, space_raw, turn_raw, left_out, left_in, left_next,
    field, bonds, shifted, pack_out, pack_in, loop_rows, loop_out, loop_in,
    oper, chain_a, chain_b, group, sums, final,
    in_sem, edge_out, edge_in, halo_out, halo_in, loop_sent, loop_got, local_sem, back_sem, done_sem,
    known,
):
    ix, iz, ia = lax.axis_index("ta_0"), lax.axis_index("ta_1"), lax.axis_index("sa")
    nx, nz, na = 4, 4, lax.axis_size("sa")
    left, right = lax.rem(ia + na - 1, na), lax.rem(ia + 1, na)
    slab = ix * nz + iz
    earlier = lax.rem(slab + nx * nz - 1, nx * nz)
    later = lax.rem(slab + 1, nx * nz)
    earlier_x, earlier_z = earlier // nz, lax.rem(earlier, nz)
    later_x, later_z = later // nz, lax.rem(later, nz)
    halves = 2 * SWEEPS

    for t in range(4):
        for j in range(3):
            lanes, rows = pl.ds(LANES * j, LANES), pl.ds(8 * t + 2 * j, 2)
            pltpu.make_async_copy(
                time_hbm.at[:, t, :, lanes], time_raw.at[:, rows, :], in_sem.at[0]).start()
    for t in range(4):
        for j in range(3):
            lanes, rows = pl.ds(LANES * j, LANES), pl.ds(8 * t + 2 * j, 2)
            pltpu.make_async_copy(
                space_hbm.at[:, :, t, :, lanes], space_raw.at[:, :, rows, :], in_sem.at[1]).start()
    for t in range(4):
        for j in range(3):
            lanes, rows = pl.ds(LANES * j, LANES), pl.ds(8 * t + 2 * j, 2)
            pltpu.make_async_copy(
                turn_hbm.at[:, :, :, t, :, lanes], turn_raw.at[:, :, :, rows, :], in_sem.at[2]
            ).start()

    barrier = pltpu.get_barrier_semaphore()
    peers = [(ix, iz, left), (ix, iz, right)]
    peers += [(earlier_x, earlier_z, ia), (later_x, later_z, ia)]
    peers += [(earlier_x, earlier_z, right), (later_x, later_z, left)]
    for peer in peers:
        pl.semaphore_signal(barrier, inc=1, device_id=peer, device_id_type=MESH)

    def remote(src, dst, out_sem, got_sem, target):
        return pltpu.make_async_remote_copy(
            src_ref=src, dst_ref=dst, send_sem=out_sem, recv_sem=got_sem,
            device_id=target, device_id_type=MESH)

    def landed(ref, sem):
        pltpu.make_async_copy(ref, ref, sem).wait()

    def tell(stage):
        for side, step in ((0, 1 << stage), (1, nx * nz - (1 << stage))):
            peer = lax.rem(slab + step, nx * nz)
            pl.semaphore_signal(
                known.at[stage, side], inc=1, device_id=(peer // nz, lax.rem(peer, nz), ia),
                device_id_type=MESH)

    def hear(stage):
        for side in range(2):
            pl.semaphore_wait(known.at[stage, side], 1)

    shifts = Shifts()
    odd = shifts.odd

    def own(parity, first, second):
        return jnp.where(odd, first, second) if parity else jnp.where(odd, second, first)

    def split(values):
        return values[:9], values[9:]

    def pack(number, block, parity, links):
        for k in range(9):
            real, partner = links[0][k], shifts.pair_swap(links[1][k])
            pack_out[number, block, 0, k] = own(parity, real, partner)
            pack_out[number, block, 1, k] = own(parity, partner, real)

    def send_halo(number, block, side, target):
        for at in (0, 4):
            rows = pl.ds(at, 3)
            remote(
                pack_out.at[number, block, side, :, rows, :],
                pack_in.at[number, block, side, :, rows, :],
                halo_out.at[number, block, side], halo_in.at[number, block, side],
                (ix, iz, target)).start()

    def await_halo(sem, number, block, side):
        landed(pack_in.at[number, block, side, :, pl.ds(0, 6), :], sem.at[number, block, side])

    two_rows = [*range(6), *range(9, 15)]
    landed(time_raw.at[:, pl.ds(0, 24), :], in_sem.at[0])
    for block in range(2):
        packed = []
        for entry in range(18):
            first = time_raw[entry, pl.ds(16 * block, 8, stride=2), :]
            second = time_raw[entry, pl.ds(16 * block + 1, 8, stride=2), :]
            field[0, entry, pl.ds(8 * block, 8), :] = own(0, first, second)
            value = own(1, first, second)
            field[1, entry, pl.ds(8 * block, 8), :] = value
            packed.append(value)
        pack(0, block, 1, split(packed))
    pl.semaphore_wait(barrier, len(peers))
    for block in range(2):
        for side, target in ((0, left), (1, right)):
            send_halo(0, block, side, target)
    landed(space_raw.at[:, :, pl.ds(0, 24), :], in_sem.at[1])
    for block in range(2):
        for place, entry in enumerate(two_rows):
            left_out[place, pl.ds(8 * block, 8), :] = (
                space_raw[0, entry, pl.ds(16 * block + 1, 8, stride=2), :])
    edges = []
    for t in range(4):
        rows = pl.ds(4 * t, 3)
        edges.append(remote(
            left_out.at[:, rows, :], left_in.at[:, rows, :], edge_out.at[0], edge_in.at[0],
            (ix, iz, right)))
    for half in range(2):
        rows = pl.ds(0, 6)
        edges.append(remote(
            space_raw.at[:, pl.ds(9 * half, 6), rows, :],
            space_raw.at[:, pl.ds(9 * half, 6), pl.ds(32, 6), :],
            edge_out.at[1 + half], edge_in.at[1 + half], (earlier_x, earlier_z, ia)))
    edges.append(remote(
        left_out.at[:, pl.ds(0, 3), :], left_next.at[:, pl.ds(0, 3), :],
        edge_out.at[3], edge_in.at[3], (earlier_x, earlier_z, right)))
    for copy in edges:
        copy.start()
    tell(0)
    covers = (
        left_in.at[:, pl.ds(0, 12), :], space_raw.at[:, pl.ds(0, 6), pl.ds(0, 6), :],
        space_raw.at[:, pl.ds(0, 6), pl.ds(0, 6), :], left_in.at[:, pl.ds(0, 3), :])

    def raw(direction, at, column):
        return [space_raw[direction, k, pl.ds(at + column, 8, stride=2), :] for k in range(18)]

    def inner_bonds(block):
        at, to = 16 * block, pl.ds(8 * block, 8)
        if not isinstance(block, int):
            at, to = pl.multiple_of(at, 16), pl.ds(pl.multiple_of(8 * block, 8), 8)

        def put(parity, place, matrix):
            for k in range(9):
                bonds[parity, place, k, to, :] = matrix[0][k]
                bonds[parity, place, 9 + k, to, :] = matrix[1][k]

        inner = raw(0, at, 0)
        inner_dag = dagger(split(inner))
        inner_dag = inner_dag[0] + inner_dag[1]
        for parity in (0, 1):
            put(parity, 0, split([own(parity, a, b) for a, b in zip(inner, inner_dag)]))
        for direction, shift in ((1, shifts.rows), (2, shifts.deep)):
            first, second = raw(direction, at, 0), raw(direction, at, 1)
            for parity in (0, 1):
                here = [own(parity, a, b) for a, b in zip(first, second)]
                put(parity, 2 * direction - 1, split(here))
                back = [shift(value, -1) for value in here]
                put(1 - parity, 2 * direction, dagger(split(back)))

    def outer_bonds(block):
        to = pl.ds(8 * block, 8)
        outer = raw(0, 16 * block, 1)
        if block < 2:
            six = [left_in[k, to, :] for k in range(12)]
        else:
            six = [left_next[k] for k in range(12)]
        beyond = dagger(closed((six[:6], six[6:])))
        beyond = beyond[0] + beyond[1]
        for parity in (0, 1):
            for k in range(18):
                bonds[parity, 5, k, to, :] = own(parity, beyond[k], outer[k])

    @pl.loop(0, 2)
    def _(block):
        inner_bonds(block)

    landed(turn_raw.at[:, :, :, pl.ds(0, 24), :], in_sem.at[2])
    landed(covers[0], edge_in.at[0])
    for block in range(2):
        outer_bonds(block)
    hear(0)
    tell(1)

    def half_sweep(sweep, parity):
        number = 2 * sweep + parity

        @pl.loop(0, 2)
        def _(block):
            rows = pl.ds(pl.multiple_of(8 * block, 8), 8)
            rows_later = pl.ds(8 * block + 4, 8)

            if parity == 0:
                @pl.when(jnp.logical_and(sweep == 0, block == 1))
                def _():
                    for piece in range(1, 4):
                        landed(covers[piece], edge_in.at[piece])
                    hear(1)
                    tell(2)
                    for direction in range(3):
                        six = [space_raw[direction, k, pl.ds(32, 8), :] for k in two_rows]
                        re, im = closed((six[:6], six[6:]))
                        for k in range(6, 9):
                            space_raw[direction, k, pl.ds(32, 8), :] = re[k]
                            space_raw[direction, 9 + k, pl.ds(32, 8), :] = im[k]
                    inner_bonds(2)
                    outer_bonds(2)

            def load(ref, lead, where):
                return split([ref[(*lead, k, where, slice(None))] for k in range(18)])

            for entry in range(18):
                value = field[1 - parity, entry, rows, :]
                shifted[0, entry] = shifts.rows(value, 1)
                shifted[1, entry] = shifts.rows(value, -1)
                shifted[2, entry] = shifts.deep(value, 1)
                shifted[3, entry] = shifts.deep(value, -1)
            total = ([None] * 9, [None] * 9)
            total = staple_term(
                total, load(bonds, (parity, 0), rows_later), load(bonds, (parity, 0), rows),
                load(field, (1 - parity,), rows))
            for place in range(1, 5):
                total = staple_term(
                    total, load(bonds, (parity, place), rows_later),
                    load(bonds, (parity, place), rows),
                    load(shifted, (place - 1,), slice(None)))

            for side in range(2):
                await_halo(halo_in, number, block, side)
            beyond_re, beyond_im = [], []
            for k in range(9):
                from_left = pack_in[number, block, 1, k]
                from_right = pack_in[number, block, 0, k]
                beyond_re.append(own(parity, from_left, from_right))
                beyond_im.append(shifts.pair_swap(own(parity, from_right, from_left)))
            total = staple_term(
                total, load(bonds, (parity, 5), rows_later), load(bonds, (parity, 5), rows),
                (beyond_re, beyond_im))
            links = load(field, (parity,), rows)
            product = times(links, total)
            for plane, (upper, lower) in enumerate(PLANES):
                base = pl.multiple_of(16 * block, 16)
                turn = [
                    own(parity, turn_raw[sweep, plane, k, pl.ds(base, 8, stride=2), :],
                        turn_raw[sweep, plane, k, pl.ds(base + 1, 8, stride=2), :])
                    for k in range(4)]
                quat = reflected(product, upper, lower, turn)
                links = rotate_rows(links, upper, lower, quat)
                if plane < 2:
                    product = rotate_rows(product, upper, lower, quat)
            for k in range(9):
                field[parity, k, rows, :] = links[0][k]
                field[parity, 9 + k, rows, :] = links[1][k]

            @pl.when(number < halves - 1)
            def _():
                pack(number + 1, block, parity, links)
                for side, target in ((0, left), (1, right)):
                    send_halo(number + 1, block, side, target)

    def send_loops(sweep, parity):
        low = shifts.low_rows
        number = 2 * sweep + parity
        even, uneven = [], []
        for entry in range(18):
            a = field[parity, entry, pl.ds(0, 8), :]
            b = field[parity, entry, pl.ds(4, 8), :]
            c = field[parity, entry, pl.ds(8, 8), :]
            even.append(jnp.where(low, a, b))
            uneven.append(jnp.where(low, b, c))
        re, im = times(split(even), split(uneven))
        re, im = times((re, im), ([turn_rows(v, 4) for v in re], [turn_rows(v, 4) for v in im]))
        for entry, value in enumerate(re + im):
            loop_rows[pl.ds(8 * entry, 8), :] = value
        for j in range(3):
            for third in range(3):
                loop_out[number, j, pl.ds(8 * third, 8), :] = (
                    loop_rows[pl.ds(64 * third + j, 8, stride=8), :])

        def loop_to(peer_x):
            at = pl.multiple_of(24 * (2 * ix + parity), 8)
            return (
                loop_out.at[number, peer_x - 1, pl.ds(0, 18), :],
                loop_in.at[sweep, iz, pl.ds(at, 18), :])

        for step_z, step_x in [(z, x) for z in (2, 1, 3, 0) for x in (2, 1, 3, 0)]:
            if step_z == step_x == 0:
                @pl.when(ix > 0)
                def _():
                    pltpu.make_async_copy(*loop_to(ix), local_sem.at[number]).start()
            else:
                peer_x, peer_z = lax.rem(ix + step_x, nx), lax.rem(iz + step_z, nz)

                @pl.when(peer_x > 0)
                def _():
                    remote(
                        *loop_to(peer_x), loop_sent.at[number], loop_got.at[number],
                        (peer_x, peer_z, ia)).start()

    @pl.loop(0, SWEEPS)
    def _(sweep):
        for parity in (0, 1):
            half_sweep(sweep, parity)
            if parity == 0:
                @pl.when(sweep == 0)
                def _():
                    hear(2)
            send_loops(sweep, parity)

    def normalized(load, store, log):
        squares = [load(k) * load(k) for k in range(6)]
        for k in range(6, 162):
            value = load(k)
            squares[k % 6] = squares[k % 6] + value * value
        square = (squares[0] + squares[1]) + (squares[2] + squares[3]) + (squares[4] + squares[5])
        rms = jnp.sqrt(square / 162.0 + 1e-06)
        inv = 1.0 / rms
        for k in range(162):
            store(k, load(k) * inv)
        return log + jnp.log(rms)

    def combine(left_ref, right_ref, dst_ref, keep):
        for k in range(81):
            sums[k] = right_ref[k] + right_ref[81 + k]

        @pl.loop(0, 9)
        def _(row):
            for third in range(3):
                columns = range(3 * third, 3 * third + 3)
                acc = [[None] * 3 for _ in columns]
                for mid in range(9):
                    a_re, a_im = left_ref[9 * row + mid], left_ref[81 + 9 * row + mid]
                    a_sum = a_re + a_im
                    for place, col in enumerate(columns):
                        at = 9 * mid + col
                        terms = (a_re * right_ref[at], a_im * right_ref[81 + at], a_sum * sums[at])
                        for slot, term in enumerate(terms):
                            old = acc[place][slot]
                            acc[place][slot] = term if old is None else old + term
                for place, col in enumerate(columns):
                    plain, cross, both = acc[place]
                    dst_ref[9 * row + col] = plain - cross
                    dst_ref[81 + 9 * row + col] = both - plain - cross
        log = normalized(
            lambda k: dst_ref[k], lambda k, value: dst_ref.__setitem__(k, keep(k, value)),
            left_ref[162] + right_ref[162])
        dst_ref[162] = keep(162, log)

    def result_to(target):
        lanes = pl.ds(pl.multiple_of(LANES * (ix - 1), LANES), LANES)
        rows = pl.ds(2 * target, 2)
        return (
            (final.at[pl.ds(0, 162), rows, :], out_hbm.at[:, :, lanes]),
            (final.at[162, rows, :], log_hbm.at[:, lanes]))

    @pl.when(ix > 0)
    def _():
        def await_loops(number):
            ref = loop_out.at[number, 0, pl.ds(0, 18), :]
            landed(ref, local_sem.at[number])
            landed(space_raw.at[0, :, pl.ds(0, 15), :], loop_got.at[number])

        def add_operator(slot, sweep):
            to = jnp.where(slot == 0, 0, slot + 3)
            loops = [loop_in[sweep, slot, pl.ds(k, 8, stride=24), :] for k in range(18)]
            partner = [shifts.deep(value, 4) for value in loops]
            for a in range(3):
                for c in range(3):
                    for e in range(3):
                        for d in range(3):
                            l_re, l_im = loops[3 * a + e], loops[9 + 3 * a + e]
                            r_re, r_im = partner[3 * c + d], partner[9 + 3 * c + d]
                            re = l_re * r_re + l_im * r_im
                            im = l_im * r_re - l_re * r_im
                            at = 9 * (3 * a + c) + 3 * e + d
                            if sweep:
                                re = oper[to, at] + re
                                im = oper[to, 81 + at] + im
                            oper[to, at] = re
                            oper[to, 81 + at] = im
            return to

        for sweep in range(SWEEPS):
            await_loops(2 * sweep)
            await_loops(2 * sweep + 1)

            @pl.loop(0, nz)
            def _(slot):
                to = add_operator(slot, sweep)
                if sweep == SWEEPS - 1:
                    third = 1.0 / SWEEPS
                    log = normalized(
                        lambda k: oper[to, k] * third,
                        lambda k, value: oper.at[to].__setitem__(k, value),
                        jnp.zeros((8, LANES)))
                    oper[to, 162] = log

        @pl.loop(1, nz)
        def _(slot):
            combine(oper.at[slot - 1], oper.at[slot + 3], oper.at[slot], lambda k, value: value)

        row = lax.broadcasted_iota(jnp.int32, (8, LANES), 0)

        def moved(value, k, rows):
            unit = 1.0 if k < 81 and k % 10 == 0 else 0.0
            return jnp.where(row < rows, unit, turn_rows(value, -rows))

        def by_column(k, value):
            swapped = jnp.where(row % 2 == 0, turn_rows(value, 1), turn_rows(value, -1))
            return jnp.where(odd, swapped, value)

        for k in range(163):
            chain_a[k] = moved(oper[nz - 1, k], k, 2)
            chain_b[k] = moved(chain_a[k], k, 2)
        combine(chain_b, chain_a, group, lambda k, value: jnp.where(row < 2, chain_a[k], value))
        for k in range(163):
            chain_b[k] = moved(group[k], k, 4)
        combine(chain_b, group, chain_a, lambda k, value: jnp.where(row < 4, group[k], value))
        combine(chain_a, oper.at[iz], final, by_column)

        for target in range(nx):
            @pl.when(ix == target)
            def _():
                for piece, (src, dst) in enumerate(result_to(target)):
                    pltpu.make_async_copy(src, dst, done_sem.at[piece]).start()

            @pl.when(ix != target)
            def _():
                for piece, (src, dst) in enumerate(result_to(target)):
                    remote(
                        src, dst, done_sem.at[2 + piece], back_sem.at[piece, ix], (target, iz, ia)
                    ).start()
        for piece, (src, dst) in enumerate(result_to(0)):
            pltpu.make_async_copy(src, dst, done_sem.at[piece]).wait()

    for source in range(1, nx):
        @pl.when(ix != source)
        def _():
            landed(final.at[pl.ds(0, 162), pl.ds(0, 2), :], back_sem.at[0, source])
            landed(final.at[162, pl.ds(0, 2), :], back_sem.at[1, source])

    for piece, cover in enumerate(covers):
        landed(cover, edge_out.at[piece])
    for number in range(halves):
        for block in range(2):
            for side in range(2):
                await_halo(halo_out, number, block, side)

    @pl.when(ix == 0)
    def _():
        for number in range(halves):
            landed(space_raw.at[0, :, pl.ds(0, 12), :], loop_sent.at[number])

    @pl.when(ix > 0)
    def _():
        for number in range(halves):
            landed(space_raw.at[0, :, pl.ds(0, 11), :], loop_sent.at[number])
        landed(final.at[pl.ds(0, 162), pl.ds(0, 6), :], done_sem.at[2])
        landed(final.at[162, pl.ds(0, 6), :], done_sem.at[3])


def per_device(temporal_links, spatial_links, rotations):
    f32, dma = jnp.float32, pltpu.SemaphoreType.DMA
    halves = 2 * SWEEPS
    transfer, log_scale = pl.pallas_call(
        kernel,
        name="slab_chain",
        out_shape=(pltpu.VMEM((162, 2, 3 * LANES), f32), pltpu.VMEM((2, 3 * LANES), f32)),
        in_specs=[pl.BlockSpec(memory_space=pl.ANY)] * 3,
        out_specs=[pl.BlockSpec(memory_space=pltpu.VMEM)] * 2,
        scratch_shapes=[
            pltpu.VMEM((18, 32, LANES), f32),
            pltpu.VMEM((3, 18, 48, LANES), f32),
            pltpu.VMEM((3, 3, 4, 32, LANES), f32),
            pltpu.VMEM((12, 16, LANES), f32),
            pltpu.VMEM((12, 16, LANES), f32),
            pltpu.VMEM((12, 8, LANES), f32),
            pltpu.VMEM((2, 18, 16, LANES), f32),
            pltpu.VMEM((2, 6, 18, 24, LANES), f32),
            pltpu.VMEM((4, 18, 8, LANES), f32),
            pltpu.VMEM((halves, 2, 2, 9, 8, LANES), f32),
            pltpu.VMEM((halves, 2, 2, 9, 8, LANES), f32),
            pltpu.VMEM((192, LANES), f32),
            pltpu.VMEM((halves, 3, 24, LANES), f32),
            pltpu.VMEM((SWEEPS, 4, 192, LANES), f32),
            pltpu.VMEM((7, 163, 8, LANES), f32),
            pltpu.VMEM((163, 8, LANES), f32),
            pltpu.VMEM((163, 8, LANES), f32),
            pltpu.VMEM((163, 8, LANES), f32),
            pltpu.VMEM((81, 8, LANES), f32),
            pltpu.VMEM((163, 8, LANES), f32),
            dma((3,)), dma((4,)), dma((4,)), dma((halves, 2, 2)), dma((halves, 2, 2)),
            dma((halves,)), dma((halves,)), dma((halves,)), dma((2, 4)), dma((4,)),
            pltpu.SemaphoreType.REGULAR((3, 2)),
        ],
        compiler_params=pltpu.CompilerParams(collective_id=0, has_side_effects=True),
    )(temporal_links, spatial_links, rotations)
    return transfer.reshape(2, 9, 9, 1, 2, 3 * LANES), log_scale.reshape(1, 2, 3 * LANES)


def solution(mesh):
    split = Mesh(mesh.devices.reshape(4, 4, mesh.shape["sa"]), AXES)
    slabs = ("ta_0", "ta_1")
    return jax.shard_map(
        per_device,
        mesh=split,
        in_specs=(
            P(None, slabs, "sa", None),
            P(None, None, slabs, "sa", None),
            P(None, None, None, slabs, "sa", None),
        ),
        out_specs=(P(None, None, None, slabs, "sa", None), P(slabs, "sa", None)),
        check_vma=False,
    )
```

```python
import jax
import jax.numpy as jnp
from jax import lax
from jax.experimental import pallas as pl
from jax.experimental.pallas import tpu as pltpu
from jax.sharding import Mesh
from jax.sharding import PartitionSpec as P

SWEEPS = 3
LZ = 16
LANES = 128
MESH = pl.DeviceIdType.MESH
AXES = ("ta_0", "ta_1", "sa")
PLANES = ((0, 1), (1, 2), (0, 2))


def times(left, right):
    out_re, out_im = [], []
    for row in range(3):
        for col in range(3):
            re = im = None
            for mid in range(3):
                a_re, a_im = left[0][3 * row + mid], left[1][3 * row + mid]
                b_re, b_im = right[0][3 * mid + col], right[1][3 * mid + col]
                p_re = a_re * b_re - a_im * b_im
                p_im = a_re * b_im + a_im * b_re
                re = p_re if re is None else re + p_re
                im = p_im if im is None else im + p_im
            out_re.append(re)
            out_im.append(im)
    return out_re, out_im


def staple_term(total, later, now, link):
    total_re, total_im = list(total[0]), list(total[1])
    for col in range(3):
        mid_re, mid_im = [], []
        for k in range(3):
            re = im = None
            for m in range(3):
                a_re, a_im = now[0][3 * col + m], now[1][3 * col + m]
                b_re, b_im = link[0][3 * m + k], link[1][3 * m + k]
                p_re = a_re * b_re - a_im * b_im
                p_im = a_re * b_im + a_im * b_re
                re = p_re if re is None else re + p_re
                im = p_im if im is None else im + p_im
            mid_re.append(re)
            mid_im.append(im)
        for row in range(3):
            re, im = total_re[3 * row + col], total_im[3 * row + col]
            for k in range(3):
                a_re, a_im = later[0][3 * row + k], later[1][3 * row + k]
                p_re = a_re * mid_re[k] + a_im * mid_im[k]
                p_im = a_im * mid_re[k] - a_re * mid_im[k]
                re = p_re if re is None else re + p_re
                im = p_im if im is None else im + p_im
            total_re[3 * row + col], total_im[3 * row + col] = re, im
    return total_re, total_im


def dagger(matrix):
    order = (0, 3, 6, 1, 4, 7, 2, 5, 8)
    return [matrix[0][k] for k in order], [-matrix[1][k] for k in order]


def rotate_rows(matrix, upper, lower, quat):
    q0, q1, q2, q3 = quat
    re, im = list(matrix[0]), list(matrix[1])
    for col in range(3):
        u_re, u_im = matrix[0][3 * upper + col], matrix[1][3 * upper + col]
        l_re, l_im = matrix[0][3 * lower + col], matrix[1][3 * lower + col]
        re[3 * upper + col] = q0 * u_re - q3 * u_im + q2 * l_re - q1 * l_im
        im[3 * upper + col] = q0 * u_im + q3 * u_re + q2 * l_im + q1 * l_re
        re[3 * lower + col] = q0 * l_re + q3 * l_im - q2 * u_re - q1 * u_im
        im[3 * lower + col] = q0 * l_im - q3 * l_re - q2 * u_im + q1 * u_re
    return re, im


def reflected(product, upper, lower, turn):
    re, im = product
    uu, ul, lu, ll = 4 * upper, 3 * upper + lower, 3 * lower + upper, 4 * lower
    w0 = 0.5 * (re[uu] + re[ll])
    w1 = 0.5 * (im[ul] + im[lu])
    w2 = 0.5 * (re[ul] - re[lu])
    w3 = 0.5 * (im[uu] - im[ll])
    vec_sq = w1 * w1 + w2 * w2 + w3 * w3
    w0_sq = w0 * w0
    inv = 1.0 / jnp.maximum(w0_sq + vec_sq, 0.5)
    scale = -2.0 * w0 * inv
    r0, r1, r2, r3 = (w0_sq - vec_sq) * inv, scale * w1, scale * w2, scale * w3
    x0, x1, x2, x3 = turn
    return (
        x0 * r0 - (x1 * r1 + x2 * r2 + x3 * r3),
        x0 * r1 + r0 * x1 - (x2 * r3 - x3 * r2),
        x0 * r2 + r0 * x2 - (x3 * r1 - x1 * r3),
        x0 * r3 + r0 * x3 - (x1 * r2 - x2 * r1),
    )


def closed(six):
    re, im = list(six[0]), list(six[1])
    for col in range(3):
        a, b = (col + 1) % 3, (col + 2) % 3
        real = (re[a] * re[3 + b] - im[a] * im[3 + b]) - (re[b] * re[3 + a] - im[b] * im[3 + a])
        imag = (re[a] * im[3 + b] + im[a] * re[3 + b]) - (re[b] * im[3 + a] + im[b] * re[3 + a])
        re.append(real)
        im.append(-imag)
    return re, im


def turn_lanes(value, steps):
    return pltpu.roll(value, (-steps) % LANES, 1)


def turn_rows(value, steps):
    return pltpu.roll(value, (-steps) % 8, 0)


class Shifts:
    def __init__(self):
        lane = lax.broadcasted_iota(jnp.int32, (8, LANES), 1)
        row = lax.broadcasted_iota(jnp.int32, (8, LANES), 0)
        self.depth = lane % LZ
        self.lane = lane
        self.slot = row % 4
        self.odd = ((lane // LZ + lane) % 2) == 1
        self.low_rows = row < 4
        self.even_lane = lane % 2 == 0

    def rows(self, value, offset):
        if offset > 0:
            turned = turn_lanes(value, LZ)
            after = jnp.where(self.slot == 2, turn_rows(turned, -2), turn_rows(turned, 1))
            return jnp.where(self.lane < LANES - LZ, turned, after)
        turned = turn_lanes(value, -LZ)
        before = jnp.where(self.slot == 0, turn_rows(turned, 2), turn_rows(turned, -1))
        return jnp.where(self.lane >= LZ, turned, before)

    def deep(self, value, offset):
        if offset > 0:
            return jnp.where(
                self.depth < LZ - offset, turn_lanes(value, offset), turn_lanes(value, offset - LZ)
            )
        return jnp.where(
            self.depth >= -offset, turn_lanes(value, offset), turn_lanes(value, LZ + offset)
        )

    def pair_swap(self, value):
        return jnp.where(self.even_lane, turn_lanes(value, 1), turn_lanes(value, -1))


def kernel(
    time_hbm, space_hbm, turn_hbm, out_hbm, log_hbm,
    time_raw, space_raw, turn_raw, left_out, left_in, left_next,
    field, bonds, shifted, pack_out, pack_in, loop_rows, loop_out, loop_in,
    oper, chain_a, chain_b, group, sums, final,
    in_sem, edge_out, edge_in, halo_out, halo_in, loop_sent, loop_got, local_sem, back_sem, done_sem,
    known,
):
    ix, iz, ia = lax.axis_index("ta_0"), lax.axis_index("ta_1"), lax.axis_index("sa")
    nx, nz, na = 4, 4, lax.axis_size("sa")
    left, right = lax.rem(ia + na - 1, na), lax.rem(ia + 1, na)
    slab = ix * nz + iz
    earlier = lax.rem(slab + nx * nz - 1, nx * nz)
    later = lax.rem(slab + 1, nx * nz)
    earlier_x, earlier_z = earlier // nz, lax.rem(earlier, nz)
    later_x, later_z = later // nz, lax.rem(later, nz)
    halves = 2 * SWEEPS

    for t in range(4):
        for j in range(3):
            lanes, rows = pl.ds(LANES * j, LANES), pl.ds(8 * t + 2 * j, 2)
            pltpu.make_async_copy(
                time_hbm.at[:, t, :, lanes], time_raw.at[:, rows, :], in_sem.at[0]).start()
    for t in range(4):
        for j in range(3):
            lanes, rows = pl.ds(LANES * j, LANES), pl.ds(8 * t + 2 * j, 2)
            pltpu.make_async_copy(
                space_hbm.at[:, :, t, :, lanes], space_raw.at[:, :, rows, :], in_sem.at[1]).start()
    for t in range(4):
        for j in range(3):
            lanes, rows = pl.ds(LANES * j, LANES), pl.ds(8 * t + 2 * j, 2)
            pltpu.make_async_copy(
                turn_hbm.at[:, :, :, t, :, lanes], turn_raw.at[:, :, :, rows, :], in_sem.at[2]
            ).start()

    barrier = pltpu.get_barrier_semaphore()
    peers = [(ix, iz, left), (ix, iz, right)]
    peers += [(earlier_x, earlier_z, ia), (later_x, later_z, ia)]
    peers += [(earlier_x, earlier_z, right), (later_x, later_z, left)]
    for peer in peers:
        pl.semaphore_signal(barrier, inc=1, device_id=peer, device_id_type=MESH)

    def remote(src, dst, out_sem, got_sem, target):
        return pltpu.make_async_remote_copy(
            src_ref=src, dst_ref=dst, send_sem=out_sem, recv_sem=got_sem,
            device_id=target, device_id_type=MESH)

    def landed(ref, sem):
        pltpu.make_async_copy(ref, ref, sem).wait()

    def tell(stage):
        for side, step in ((0, 1 << stage), (1, nx * nz - (1 << stage))):
            peer = lax.rem(slab + step, nx * nz)
            pl.semaphore_signal(
                known.at[stage, side], inc=1, device_id=(peer // nz, lax.rem(peer, nz), ia),
                device_id_type=MESH)

    def hear(stage):
        for side in range(2):
            pl.semaphore_wait(known.at[stage, side], 1)

    shifts = Shifts()
    odd = shifts.odd

    def own(parity, first, second):
        return jnp.where(odd, first, second) if parity else jnp.where(odd, second, first)

    def split(values):
        return values[:9], values[9:]

    def pack(number, block, parity, links):
        for k in range(9):
            real, partner = links[0][k], shifts.pair_swap(links[1][k])
            pack_out[number, block, 0, k] = own(parity, real, partner)
            pack_out[number, block, 1, k] = own(parity, partner, real)

    def send_halo(number, block, side, target):
        for at in (0, 4):
            rows = pl.ds(at, 3)
            remote(
                pack_out.at[number, block, side, :, rows, :],
                pack_in.at[number, block, side, :, rows, :],
                halo_out.at[number, block, side], halo_in.at[number, block, side],
                (ix, iz, target)).start()

    def await_halo(sem, number, block, side):
        landed(pack_in.at[number, block, side, :, pl.ds(0, 6), :], sem.at[number, block, side])

    two_rows = [*range(6), *range(9, 15)]
    landed(time_raw.at[:, pl.ds(0, 24), :], in_sem.at[0])
    for block in range(2):
        packed = []
        for entry in range(18):
            first = time_raw[entry, pl.ds(16 * block, 8, stride=2), :]
            second = time_raw[entry, pl.ds(16 * block + 1, 8, stride=2), :]
            field[0, entry, pl.ds(8 * block, 8), :] = own(0, first, second)
            value = own(1, first, second)
            field[1, entry, pl.ds(8 * block, 8), :] = value
            packed.append(value)
        pack(0, block, 1, split(packed))
    pl.semaphore_wait(barrier, len(peers))
    for block in range(2):
        for side, target in ((0, left), (1, right)):
            send_halo(0, block, side, target)
    landed(space_raw.at[:, :, pl.ds(0, 24), :], in_sem.at[1])
    for block in range(2):
        for place, entry in enumerate(two_rows):
            left_out[place, pl.ds(8 * block, 8), :] = (
                space_raw[0, entry, pl.ds(16 * block + 1, 8, stride=2), :])
    edges = []
    for t in range(4):
        rows = pl.ds(4 * t, 3)
        edges.append(remote(
            left_out.at[:, rows, :], left_in.at[:, rows, :], edge_out.at[0], edge_in.at[0],
            (ix, iz, right)))
    for half in range(2):
        rows = pl.ds(0, 6)
        edges.append(remote(
            space_raw.at[:, pl.ds(9 * half, 6), rows, :],
            space_raw.at[:, pl.ds(9 * half, 6), pl.ds(32, 6), :],
            edge_out.at[1 + half], edge_in.at[1 + half], (earlier_x, earlier_z, ia)))
    edges.append(remote(
        left_out.at[:, pl.ds(0, 3), :], left_next.at[:, pl.ds(0, 3), :],
        edge_out.at[3], edge_in.at[3], (earlier_x, earlier_z, right)))
    for copy in edges:
        copy.start()
    tell(0)
    covers = (
        left_in.at[:, pl.ds(0, 12), :], space_raw.at[:, pl.ds(0, 6), pl.ds(0, 6), :],
        space_raw.at[:, pl.ds(0, 6), pl.ds(0, 6), :], left_in.at[:, pl.ds(0, 3), :])

    def raw(direction, at, column):
        return [space_raw[direction, k, pl.ds(at + column, 8, stride=2), :] for k in range(18)]

    def inner_bonds(block):
        at, to = 16 * block, pl.ds(8 * block, 8)
        if not isinstance(block, int):
            at, to = pl.multiple_of(at, 16), pl.ds(pl.multiple_of(8 * block, 8), 8)

        def put(parity, place, matrix):
            for k in range(9):
                bonds[parity, place, k, to, :] = matrix[0][k]
                bonds[parity, place, 9 + k, to, :] = matrix[1][k]

        inner = raw(0, at, 0)
        inner_dag = dagger(split(inner))
        inner_dag = inner_dag[0] + inner_dag[1]
        for parity in (0, 1):
            put(parity, 0, split([own(parity, a, b) for a, b in zip(inner, inner_dag)]))
        for direction, shift in ((1, shifts.rows), (2, shifts.deep)):
            first, second = raw(direction, at, 0), raw(direction, at, 1)
            for parity in (0, 1):
                here = [own(parity, a, b) for a, b in zip(first, second)]
                put(parity, 2 * direction - 1, split(here))
                back = [shift(value, -1) for value in here]
                put(1 - parity, 2 * direction, dagger(split(back)))

    def outer_bonds(block):
        to = pl.ds(8 * block, 8)
        outer = raw(0, 16 * block, 1)
        if block < 2:
            six = [left_in[k, to, :] for k in range(12)]
        else:
            six = [left_next[k] for k in range(12)]
        beyond = dagger(closed((six[:6], six[6:])))
        beyond = beyond[0] + beyond[1]
        for parity in (0, 1):
            for k in range(18):
                bonds[parity, 5, k, to, :] = own(parity, beyond[k], outer[k])

    @pl.loop(0, 2)
    def _(block):
        inner_bonds(block)

    landed(turn_raw.at[:, :, :, pl.ds(0, 24), :], in_sem.at[2])
    landed(covers[0], edge_in.at[0])
    for block in range(2):
        outer_bonds(block)
    hear(0)
    tell(1)

    def half_sweep(sweep, parity):
        number = 2 * sweep + parity

        @pl.loop(0, 2)
        def _(block):
            rows = pl.ds(pl.multiple_of(8 * block, 8), 8)
            rows_later = pl.ds(8 * block + 4, 8)

            if parity == 0:
                @pl.when(jnp.logical_and(sweep == 0, block == 1))
                def _():
                    for piece in range(1, 4):
                        landed(covers[piece], edge_in.at[piece])
                    hear(1)
                    tell(2)
                    for direction in range(3):
                        six = [space_raw[direction, k, pl.ds(32, 8), :] for k in two_rows]
                        re, im = closed((six[:6], six[6:]))
                        for k in range(6, 9):
                            space_raw[direction, k, pl.ds(32, 8), :] = re[k]
                            space_raw[direction, 9 + k, pl.ds(32, 8), :] = im[k]
                    inner_bonds(2)
                    outer_bonds(2)

            def load(ref, lead, where):
                return split([ref[(*lead, k, where, slice(None))] for k in range(18)])

            for entry in range(18):
                value = field[1 - parity, entry, rows, :]
                shifted[0, entry] = shifts.rows(value, 1)
                shifted[1, entry] = shifts.rows(value, -1)
                shifted[2, entry] = shifts.deep(value, 1)
                shifted[3, entry] = shifts.deep(value, -1)
            total = ([None] * 9, [None] * 9)
            total = staple_term(
                total, load(bonds, (parity, 0), rows_later), load(bonds, (parity, 0), rows),
                load(field, (1 - parity,), rows))
            for place in range(1, 5):
                total = staple_term(
                    total, load(bonds, (parity, place), rows_later),
                    load(bonds, (parity, place), rows),
                    load(shifted, (place - 1,), slice(None)))

            for side in range(2):
                await_halo(halo_in, number, block, side)
            beyond_re, beyond_im = [], []
            for k in range(9):
                from_left = pack_in[number, block, 1, k]
                from_right = pack_in[number, block, 0, k]
                beyond_re.append(own(parity, from_left, from_right))
                beyond_im.append(shifts.pair_swap(own(parity, from_right, from_left)))
            total = staple_term(
                total, load(bonds, (parity, 5), rows_later), load(bonds, (parity, 5), rows),
                (beyond_re, beyond_im))
            links = load(field, (parity,), rows)
            product = times(links, total)
            for plane, (upper, lower) in enumerate(PLANES):
                base = pl.multiple_of(16 * block, 16)
                turn = [
                    own(parity, turn_raw[sweep, plane, k, pl.ds(base, 8, stride=2), :],
                        turn_raw[sweep, plane, k, pl.ds(base + 1, 8, stride=2), :])
                    for k in range(4)]
                quat = reflected(product, upper, lower, turn)
                links = rotate_rows(links, upper, lower, quat)
                if plane < 2:
                    product = rotate_rows(product, upper, lower, quat)
            for k in range(9):
                field[parity, k, rows, :] = links[0][k]
                field[parity, 9 + k, rows, :] = links[1][k]

            @pl.when(number < halves - 1)
            def _():
                pack(number + 1, block, parity, links)
                for side, target in ((0, left), (1, right)):
                    send_halo(number + 1, block, side, target)

    def send_loops(sweep, parity):
        low = shifts.low_rows
        number = 2 * sweep + parity
        even, uneven = [], []
        for entry in range(18):
            a = field[parity, entry, pl.ds(0, 8), :]
            b = field[parity, entry, pl.ds(4, 8), :]
            c = field[parity, entry, pl.ds(8, 8), :]
            even.append(jnp.where(low, a, b))
            uneven.append(jnp.where(low, b, c))
        re, im = times(split(even), split(uneven))
        re, im = times((re, im), ([turn_rows(v, 4) for v in re], [turn_rows(v, 4) for v in im]))
        for entry, value in enumerate(re + im):
            loop_rows[pl.ds(8 * entry, 8), :] = value
        for j in range(3):
            for third in range(3):
                loop_out[number, j, pl.ds(8 * third, 8), :] = (
                    loop_rows[pl.ds(64 * third + j, 8, stride=8), :])

        def loop_to(peer_x):
            at = pl.multiple_of(24 * (2 * ix + parity), 8)
            return (
                loop_out.at[number, peer_x - 1, pl.ds(0, 18), :],
                loop_in.at[sweep, iz, pl.ds(at, 18), :])

        for step_z, step_x in [(z, x) for z in (2, 1, 3, 0) for x in (2, 1, 3, 0)]:
            if step_z == step_x == 0:
                @pl.when(ix > 0)
                def _():
                    pltpu.make_async_copy(*loop_to(ix), local_sem.at[number]).start()
            else:
                peer_x, peer_z = lax.rem(ix + step_x, nx), lax.rem(iz + step_z, nz)

                @pl.when(peer_x > 0)
                def _():
                    remote(
                        *loop_to(peer_x), loop_sent.at[number], loop_got.at[number],
                        (peer_x, peer_z, ia)).start()

    @pl.loop(0, SWEEPS)
    def _(sweep):
        for parity in (0, 1):
            half_sweep(sweep, parity)
            if parity == 0:
                @pl.when(sweep == 0)
                def _():
                    hear(2)
            send_loops(sweep, parity)

    def normalized(load, store, log):
        squares = [load(k) * load(k) for k in range(6)]
        for k in range(6, 162):
            value = load(k)
            squares[k % 6] = squares[k % 6] + value * value
        square = (squares[0] + squares[1]) + (squares[2] + squares[3]) + (squares[4] + squares[5])
        rms = jnp.sqrt(square / 162.0 + 1e-06)
        inv = 1.0 / rms
        for k in range(162):
            store(k, load(k) * inv)
        return log + jnp.log(rms)

    def combine(left_ref, right_ref, dst_ref, keep):
        for k in range(81):
            sums[k] = right_ref[k] + right_ref[81 + k]

        @pl.loop(0, 9)
        def _(row):
            for third in range(3):
                columns = range(3 * third, 3 * third + 3)
                acc = [[None] * 3 for _ in columns]
                for mid in range(9):
                    a_re, a_im = left_ref[9 * row + mid], left_ref[81 + 9 * row + mid]
                    a_sum = a_re + a_im
                    for place, col in enumerate(columns):
                        at = 9 * mid + col
                        terms = (a_re * right_ref[at], a_im * right_ref[81 + at], a_sum * sums[at])
                        for slot, term in enumerate(terms):
                            old = acc[place][slot]
                            acc[place][slot] = term if old is None else old + term
                for place, col in enumerate(columns):
                    plain, cross, both = acc[place]
                    dst_ref[9 * row + col] = plain - cross
                    dst_ref[81 + 9 * row + col] = both - plain - cross
        log = normalized(
            lambda k: dst_ref[k], lambda k, value: dst_ref.__setitem__(k, keep(k, value)),
            left_ref[162] + right_ref[162])
        dst_ref[162] = keep(162, log)

    def result_to(target):
        lanes = pl.ds(pl.multiple_of(LANES * (ix - 1), LANES), LANES)
        rows, stage = pl.ds(2 * target, 2), min(target, 2)
        return (
            (final.at[stage, pl.ds(0, 162), rows, :], out_hbm.at[:, :, lanes]),
            (final.at[stage, 162, rows, :], log_hbm.at[:, lanes]))

    @pl.when(ix > 0)
    def _():
        def await_loops(number):
            ref = loop_out.at[number, 0, pl.ds(0, 18), :]
            landed(ref, local_sem.at[number])
            landed(space_raw.at[0, :, pl.ds(0, 15), :], loop_got.at[number])

        def add_operator(slot, sweep):
            to = jnp.where(slot == 0, 0, slot + 3)
            loops = [loop_in[sweep, slot, pl.ds(k, 8, stride=24), :] for k in range(18)]
            partner = [shifts.deep(value, 4) for value in loops]
            for a in range(3):
                for c in range(3):
                    for e in range(3):
                        for d in range(3):
                            l_re, l_im = loops[3 * a + e], loops[9 + 3 * a + e]
                            r_re, r_im = partner[3 * c + d], partner[9 + 3 * c + d]
                            re = l_re * r_re + l_im * r_im
                            im = l_im * r_re - l_re * r_im
                            at = 9 * (3 * a + c) + 3 * e + d
                            if sweep:
                                re = oper[to, at] + re
                                im = oper[to, 81 + at] + im
                            oper[to, at] = re
                            oper[to, 81 + at] = im
            return to

        for sweep in range(SWEEPS):
            await_loops(2 * sweep)
            await_loops(2 * sweep + 1)

            @pl.loop(0, nz)
            def _(slot):
                to = add_operator(slot, sweep)
                if sweep == SWEEPS - 1:
                    third = 1.0 / SWEEPS
                    log = normalized(
                        lambda k: oper[to, k] * third,
                        lambda k, value: oper.at[to].__setitem__(k, value),
                        jnp.zeros((8, LANES)))
                    oper[to, 162] = log

        @pl.loop(1, nz)
        def _(slot):
            combine(oper.at[slot - 1], oper.at[slot + 3], oper.at[slot], lambda k, value: value)

        row = lax.broadcasted_iota(jnp.int32, (8, LANES), 0)

        def moved(value, k, rows):
            unit = 1.0 if k < 81 and k % 10 == 0 else 0.0
            return jnp.where(row < rows, unit, turn_rows(value, -rows))

        def by_column(k, value):
            swapped = jnp.where(row % 2 == 0, turn_rows(value, 1), turn_rows(value, -1))
            return jnp.where(odd, swapped, value)

        def send_result(target):
            @pl.when(ix == target)
            def _():
                for piece, (src, dst) in enumerate(result_to(target)):
                    pltpu.make_async_copy(src, dst, done_sem.at[piece]).start()

            @pl.when(ix != target)
            def _():
                for piece, (src, dst) in enumerate(result_to(target)):
                    remote(
                        src, dst, done_sem.at[2 + piece], back_sem.at[piece, ix], (target, iz, ia)
                    ).start()

        for k in range(163):
            chain_a[k] = moved(oper[nz - 1, k], k, 2)
        combine(chain_a, oper.at[iz], group, lambda k, value: value)
        for k in range(163):
            final[0, k] = by_column(k, group[k])
        send_result(0)
        for k in range(163):
            chain_b[k] = moved(chain_a[k], k, 2)
        combine(chain_b, group, chain_a, lambda k, value: value)
        for k in range(163):
            final[1, k] = by_column(k, chain_a[k])
        send_result(1)
        for k in range(163):
            group[k] = moved(chain_b[k], k, 2)
        log = normalized(
            lambda k: group[k],
            lambda k, value: group.__setitem__(k, jnp.where(row < 6, group[k], value)), group[162])
        group[162] = jnp.where(row < 6, group[162], log)
        combine(group, chain_a, final.at[2], by_column)
        send_result(2)
        send_result(3)
        for piece, (src, dst) in enumerate(result_to(0)):
            pltpu.make_async_copy(src, dst, done_sem.at[piece]).wait()

    for source in range(1, nx):
        @pl.when(ix != source)
        def _():
            landed(final.at[0, pl.ds(0, 162), pl.ds(0, 2), :], back_sem.at[0, source])
            landed(final.at[0, 162, pl.ds(0, 2), :], back_sem.at[1, source])

    for piece, cover in enumerate(covers):
        landed(cover, edge_out.at[piece])
    for number in range(halves):
        for block in range(2):
            for side in range(2):
                await_halo(halo_out, number, block, side)

    @pl.when(ix == 0)
    def _():
        for number in range(halves):
            landed(space_raw.at[0, :, pl.ds(0, 12), :], loop_sent.at[number])

    @pl.when(ix > 0)
    def _():
        for number in range(halves):
            landed(space_raw.at[0, :, pl.ds(0, 11), :], loop_sent.at[number])
        landed(final.at[0, pl.ds(0, 162), pl.ds(0, 6), :], done_sem.at[2])
        landed(final.at[0, 162, pl.ds(0, 6), :], done_sem.at[3])


def per_device(temporal_links, spatial_links, rotations):
    f32, dma = jnp.float32, pltpu.SemaphoreType.DMA
    halves = 2 * SWEEPS
    transfer, log_scale = pl.pallas_call(
        kernel,
        name="slab_chain",
        out_shape=(pltpu.VMEM((162, 2, 3 * LANES), f32), pltpu.VMEM((2, 3 * LANES), f32)),
        in_specs=[pl.BlockSpec(memory_space=pl.ANY)] * 3,
        out_specs=[pl.BlockSpec(memory_space=pltpu.VMEM)] * 2,
        scratch_shapes=[
            pltpu.VMEM((18, 32, LANES), f32),
            pltpu.VMEM((3, 18, 48, LANES), f32),
            pltpu.VMEM((3, 3, 4, 32, LANES), f32),
            pltpu.VMEM((12, 16, LANES), f32),
            pltpu.VMEM((12, 16, LANES), f32),
            pltpu.VMEM((12, 8, LANES), f32),
            pltpu.VMEM((2, 18, 16, LANES), f32),
            pltpu.VMEM((2, 6, 18, 24, LANES), f32),
            pltpu.VMEM((4, 18, 8, LANES), f32),
            pltpu.VMEM((halves, 2, 2, 9, 8, LANES), f32),
            pltpu.VMEM((halves, 2, 2, 9, 8, LANES), f32),
            pltpu.VMEM((192, LANES), f32),
            pltpu.VMEM((halves, 3, 24, LANES), f32),
            pltpu.VMEM((SWEEPS, 4, 192, LANES), f32),
            pltpu.VMEM((7, 163, 8, LANES), f32),
            pltpu.VMEM((163, 8, LANES), f32),
            pltpu.VMEM((163, 8, LANES), f32),
            pltpu.VMEM((163, 8, LANES), f32),
            pltpu.VMEM((81, 8, LANES), f32),
            pltpu.VMEM((3, 163, 8, LANES), f32),
            dma((3,)), dma((4,)), dma((4,)), dma((halves, 2, 2)), dma((halves, 2, 2)),
            dma((halves,)), dma((halves,)), dma((halves,)), dma((2, 4)), dma((4,)),
            pltpu.SemaphoreType.REGULAR((3, 2)),
        ],
        compiler_params=pltpu.CompilerParams(collective_id=0, has_side_effects=True),
    )(temporal_links, spatial_links, rotations)
    return transfer.reshape(2, 9, 9, 1, 2, 3 * LANES), log_scale.reshape(1, 2, 3 * LANES)


def solution(mesh):
    split = Mesh(mesh.devices.reshape(4, 4, mesh.shape["sa"]), AXES)
    slabs = ("ta_0", "ta_1")
    return jax.shard_map(
        per_device,
        mesh=split,
        in_specs=(
            P(None, slabs, "sa", None),
            P(None, None, slabs, "sa", None),
            P(None, None, None, slabs, "sa", None),
        ),
        out_specs=(P(None, None, None, slabs, "sa", None), P(slabs, "sa", None)),
        check_vma=False,
    )
```
